8 devices in a mesh: inst: 1 (over z), qy: 2 (over y), qx: 4 (over x, core).
Axes of the slice: x: 2, y: 2, z: 1, core: 2. Of those that a mesh axis runs over, the one named last changes fastest.
Arguments:
- cost: float32 [2097152], P(('inst', 'qy', 'qx'))
- gamma: float32 [2, 3], P('inst')
- beta: float32 [2, 3], P('inst')
Outputs:
- output 1: float32 [2], P('inst')
- output 2: float32 [2, 6], P('inst')
All inputs are finite; a program needn't handle non-finite values.
Results may differ from the reference program's by a relative error of at most 0.001.
Values sent between devices are 32-bit elements.
A program may use at most 1 GiB of HBM per device.

```python
import functools
import jax
import jax.numpy as jnp
from jax import lax

QUBITS = 21
LAYERS = 3
DEGREE = 4


def bit_table(count):
    index = jnp.arange(2 ** count, dtype=jnp.int32)[:, None]
    return ((index >> jnp.arange(count, dtype=jnp.int32)[None, :]) & 1).astype(jnp.float32)


def cut_values(adjacency):
    low_count = QUBITS // 2
    high_count = QUBITS - low_count
    low_bits = bit_table(low_count)
    high_bits = bit_table(high_count)
    degrees = jnp.sum(adjacency, axis=1)
    highest = lax.Precision.HIGHEST
    low_term = jnp.dot(low_bits, degrees[:low_count], precision=highest) - jnp.sum(jnp.dot(low_bits, adjacency[:low_count, :low_count], precision=highest) * low_bits, axis=1)
    high_term = jnp.dot(high_bits, degrees[low_count:], precision=highest) - jnp.sum(jnp.dot(high_bits, adjacency[low_count:, low_count:], precision=highest) * high_bits, axis=1)
    cross_term = jnp.dot(jnp.dot(high_bits, adjacency[low_count:, :low_count], precision=highest), low_bits.T, precision=highest)
    cut = high_term[:, None] + low_term[None, :] - 2.0 * cross_term
    total_weight = 0.5 * jnp.sum(adjacency)
    spread = jnp.sqrt(0.5 * jnp.sum(adjacency * adjacency))
    return ((cut - 0.5 * total_weight) * (2.0 / spread)).reshape(-1)


def draw_cost(cost_key):
    key_dst, key_weight = jax.random.split(cost_key)
    num_edges = QUBITS * DEGREE // 2
    edge_src = jnp.arange(num_edges, dtype=jnp.int32) % QUBITS
    edge_dst = (edge_src + jax.random.randint(key_dst, (num_edges,), 1, QUBITS)) % QUBITS
    weight_tilt = 0.5 + (edge_src + edge_dst).astype(jnp.float32) / QUBITS
    edge_weight = jax.random.uniform(key_weight, (num_edges,), jnp.float32, 0.5, 1.5) * weight_tilt
    adjacency = jnp.zeros((QUBITS, QUBITS), jnp.float32).at[edge_src, edge_dst].add(edge_weight)
    return cut_values(adjacency + adjacency.T)


def setup_inputs(seed: int = 0, part: int = 0) -> dict:
    base_key = jax.random.fold_in(jax.random.key(seed), part)
    key_cost, key_gamma, key_beta = jax.random.split(base_key, 3)
    cost = draw_cost(key_cost)
    gamma = jax.random.uniform(key_gamma, (2, LAYERS), jnp.float32, 0.2, 1.0)
    beta = jax.random.uniform(key_beta, (2, LAYERS), jnp.float32, 0.6, 2.4)
    return {"cost": cost, "gamma": gamma, "beta": beta}


def flip_bit(amplitudes, qubit):
    return jnp.flip(amplitudes.reshape(-1, 2, 2 ** qubit), axis=1).reshape(-1)


def one_set(cost, angles):
    gamma_row, beta_row = angles
    start = jnp.full(cost.shape, 2.0 ** (-0.5 * QUBITS), jnp.float32)

    def forward_layer(state, layer_angles):
        psi_re, psi_im = state
        gamma_l, beta_l = layer_angles
        phase = gamma_l * cost
        cos_p = jnp.cos(phase)
        sin_p = jnp.sin(phase)
        psi_re, psi_im = psi_re * cos_p + psi_im * sin_p, psi_im * cos_p - psi_re * sin_p
        cos_b = jnp.cos(0.5 * beta_l)
        sin_b = jnp.sin(0.5 * beta_l)
        for qubit in range(QUBITS):
            flip_re = flip_bit(psi_re, qubit)
            flip_im = flip_bit(psi_im, qubit)
            psi_re, psi_im = cos_b * psi_re + sin_b * flip_im, cos_b * psi_im - sin_b * flip_re
        return (psi_re, psi_im), None

    final_state = lax.scan(forward_layer, (start, jnp.zeros_like(start)), (gamma_row, beta_row))[0]
    psi_re, psi_im = final_state
    energy = jnp.sum(cost * (psi_re * psi_re + psi_im * psi_im))

    def backward_layer(state, layer_angles):
        psi_re, psi_im, lam_re, lam_im = state
        gamma_l, beta_l = layer_angles
        cos_b = jnp.cos(0.5 * beta_l)
        sin_b = jnp.sin(0.5 * beta_l)
        beta_grad = jnp.zeros((), jnp.float32)
        for qubit in range(QUBITS):
            flip_psi_re = flip_bit(psi_re, qubit)
            flip_psi_im = flip_bit(psi_im, qubit)
            flip_lam_re = flip_bit(lam_re, qubit)
            flip_lam_im = flip_bit(lam_im, qubit)
            beta_grad = beta_grad + jnp.sum(lam_re * flip_psi_im - lam_im * flip_psi_re)
            psi_re, psi_im = cos_b * psi_re - sin_b * flip_psi_im, cos_b * psi_im + sin_b * flip_psi_re
            lam_re, lam_im = cos_b * lam_re - sin_b * flip_lam_im, cos_b * lam_im + sin_b * flip_lam_re
        gamma_grad = 2.0 * jnp.sum(cost * (lam_re * psi_im - lam_im * psi_re))
        phase = gamma_l * cost
        cos_p = jnp.cos(phase)
        sin_p = jnp.sin(phase)
        psi_re, psi_im = psi_re * cos_p - psi_im * sin_p, psi_im * cos_p + psi_re * sin_p
        lam_re, lam_im = lam_re * cos_p - lam_im * sin_p, lam_im * cos_p + lam_re * sin_p
        return (psi_re, psi_im, lam_re, lam_im), (gamma_grad, beta_grad)

    layer_grads = lax.scan(backward_layer, (psi_re, psi_im, cost * psi_re, cost * psi_im), (gamma_row, beta_row), reverse=True)[1]
    return energy, jnp.concatenate([layer_grads[0], layer_grads[1]])


def reference(cost, gamma, beta):
    energy, grad = lax.map(functools.partial(one_set, cost), (gamma, beta))
    return (energy, grad)
```

```python
import functools
import math
import jax
import jax.numpy as jnp
from jax import lax
from jax.experimental import pallas as pl
from jax.experimental.pallas import tpu as pltpu
from jax.sharding import PartitionSpec as P

F32 = jnp.float32
BF16 = jnp.bfloat16
NK = 32
RB = 128
LN = 128
CH = 8
NCH = RB // CH
GC = 4
KG = 4
MESH = pl.DeviceIdType.MESH
LOCAL = 20


def popcount(value, bits):
    total = value % 2
    for bit in range(1, bits):
        total = total + (value // 2 ** bit) % 2
    return total


def sincos(theta):
    turns = jnp.round(theta * (1.0 / math.pi))
    red = theta - turns * 3.140625
    red = red - turns * 9.67502593994140625e-4
    red = red - turns * 1.509957990978376432e-7
    half = turns * 0.5
    sign = 1.0 - 4.0 * (half - jnp.floor(half))
    sq = red * red
    sin_p = 2.634850360e-06
    sin_p = sin_p * sq - 1.982277571e-04
    sin_p = sin_p * sq + 8.333242483e-03
    sin_p = sin_p * sq - 1.666666597e-01
    sin_v = (sin_p * sq * red + red) * sign
    cos_p = -2.629828691e-07
    cos_p = cos_p * sq + 2.477462031e-05
    cos_p = cos_p * sq - 1.388865233e-03
    cos_p = cos_p * sq + 4.166665940e-02
    cos_p = cos_p * sq - 4.999999996e-01
    cos_v = (cos_p * sq + 1.0) * sign
    return sin_v, cos_v


def butterfly(items, bits):
    shape = items.shape
    for bit in bits:
        step = 1 << bit
        pairs = items.reshape((shape[0] // (2 * step), 2, step) + shape[1:])
        first = pairs[:, 0]
        second = pairs[:, 1]
        items = jnp.stack([first + second, first - second], axis=1).reshape(shape)
    return items


def split_dot(values, table):
    high = values.astype(BF16)
    rest = values - high.astype(F32)
    mid = rest.astype(BF16)
    low = (rest - mid.astype(F32)).astype(BF16)
    parts = jnp.concatenate([high, mid, low], axis=1)
    return jnp.dot(parts, table, preferred_element_type=F32)


def kernel(cost_ref, gamma_ref, beta_ref, out_ref, cost_all, work, recv, hats, phis, had, tmp, dtab, wtab, acc, part, peers,
           own_s, own_r, rel_s, rel_r, core_s, core_r, ex_s, ex_r, fin_s, fin_r, credit):
    pos_y = lax.axis_index('qy')
    pos_b = lax.axis_index('qx')
    pos_x = pos_b // 2
    core = pos_b % 2
    other = 1 - core
    near_core = {'qy': pos_y, 'qx': pos_x * 2 + other}
    near_x = {'qy': pos_y, 'qx': (1 - pos_x) * 2 + core}
    near_y = {'qy': 1 - pos_y, 'qx': pos_b}
    near_yc = {'qy': 1 - pos_y, 'qx': pos_x * 2 + other}

    barrier = pltpu.get_barrier_semaphore()
    for dev in (near_core, near_x, near_y, near_yc):
        pl.semaphore_signal(barrier, inc=1, device_id=dev, device_id_type=MESH)
    pl.semaphore_wait(barrier, 4)

    def slot(block_y, block_x, block_core, chunk):
        return cost_all.at[block_y, block_x, pl.ds(block_core * 16 + chunk * GC, GC)]

    def push(src, dst, send, rcv, dev):
        return pltpu.make_async_remote_copy(src_ref=src, dst_ref=dst, send_sem=send, recv_sem=rcv, device_id=dev, device_id_type=MESH)

    sends = []

    def go(copy):
        copy.start()
        sends.append(copy)

    for q in range(4):
        src = cost_ref.at[pl.ds(q * GC, GC)]
        dst = slot(pos_y, pos_x, core, q)
        go(push(src, dst, own_s.at[0, q], own_r.at[0, q], near_x))
        go(push(src, dst, own_s.at[1, q], own_r.at[1, q], near_y))
        go(push(src, dst, core_s.at[0, q], core_r.at[0, q], near_core))
    cost_all[pos_y, pos_x, pl.ds(core * 16, 16)] = cost_ref[...]

    row_i = lax.broadcasted_iota(jnp.int32, (256, 256), 0)
    col_i = lax.broadcasted_iota(jnp.int32, (256, 256), 1)
    bits = row_i & col_i
    bits = bits ^ (bits >> 4)
    bits = bits ^ (bits >> 2)
    bits = bits ^ (bits >> 1)
    had_v = (1 - 2 * (bits & 1)).astype(F32).astype(BF16)
    for part_i in range(3):
        had[pl.ds(part_i * 256, 256), :] = had_v
    lane_i = lax.broadcasted_iota(jnp.int32, (8, 256), 1)
    sub_i = lax.broadcasted_iota(jnp.int32, (8, 256), 0)
    ones = sub_i & 1
    for bit in range(1, 3):
        ones = ones + ((sub_i >> bit) & 1)
    for bit in range(8):
        ones = ones + ((lane_i >> bit) & 1)
    wtab[...] = (LOCAL - 2 * ones).astype(F32)
    acc[...] = jnp.zeros_like(acc)

    for q in range(4):
        block = slot(pos_y, 1 - pos_x, core, q)
        push(block, block, own_s.at[0, q], own_r.at[0, q], near_x).wait_recv()
        go(push(block, block, core_s.at[1, q], core_r.at[1, q], near_core))
        if q < 2:
            go(push(block, block, rel_s.at[q], rel_r.at[q], near_y))
        block = slot(1 - pos_y, pos_x, core, q)
        push(block, block, own_s.at[1, q], own_r.at[1, q], near_y).wait_recv()
        go(push(block, block, core_s.at[2, q], core_r.at[2, q], near_core))
        if q >= 2:
            go(push(block, block, rel_s.at[q], rel_r.at[q], near_x))
    for q in (0, 2, 1, 3):
        block = slot(1 - pos_y, 1 - pos_x, core, q)
        push(block, block, rel_s.at[q], rel_r.at[q], near_x).wait_recv()
        go(push(block, block, core_s.at[3, q], core_r.at[3, q], near_core))
    for q in range(4):
        for kind, (by, bx) in enumerate(((pos_y, pos_x), (pos_y, 1 - pos_x), (1 - pos_y, pos_x), (1 - pos_y, 1 - pos_x))):
            block = slot(by, bx, other, q)
            push(block, block, core_s.at[kind, q], core_r.at[kind, q], near_core).wait_recv()
    for copy in sends:
        copy.wait_send()

    def make_dtab(layer, sign):
        half = 0.5 * beta_ref[pos_y, layer]
        for pop in range(10):
            sin_v, cos_v = sincos(half * (wtab[...] - 2.0 * pop))
            dtab[0, pop] = cos_v * 2.0 ** -LOCAL
            dtab[1, pop] = sin_v * (sign * 2.0 ** -LOCAL)

    def half_angle(layer):
        return sincos(jnp.full((1, CH, LN), 0.5 * beta_ref[pos_y, layer], F32))

    def cost_half(layout, half, ks, rows):
        if layout == 0:
            return cost_all[core, half, ks, rows, :]
        return cost_all[half, core, ks, rows, :]

    def radix32(src, dst):
        dst[...] = butterfly(src[...], range(5))

    def chunk_of(ref, ri, half, i):
        return ref.at[ri, half, :, pl.ds(pl.multiple_of(i * CH, CH), CH), :]

    def rchunk_of(ri, i):
        return recv.at[ri, :, pl.ds(pl.multiple_of(i * CH, CH), CH), :]

    def exchange(i):
        rows = pl.ds(pl.multiple_of(i * CH, CH), CH)
        return push(work.at[:, other, :, rows, :], recv.at[:, :, rows, :], ex_s.at[i], ex_r.at[i], near_core)

    def inner(layer):
        def body(i, carry):
            for ri in range(2):
                for half in range(2):
                    items = butterfly(work[ri, half, i].reshape(16, 8, LN), range(3))
                    tmp[ri, half] = items.reshape(RB, LN)
            rows = []
            for ri in range(2):
                cols = []
                for half in range(2):
                    items = [tmp[ri, half, pl.ds(m, 16, stride=8), :].reshape(1, 2, 8, LN) for m in range(8)]
                    items = butterfly(jnp.concatenate(items, axis=0).reshape(16, 8, LN), range(4))
                    cols.append(items.reshape(RB, LN))
                rows.append(jnp.concatenate(cols, axis=1))
            first = split_dot(jnp.concatenate(rows, axis=0), had[...])
            re_v = first[:RB]
            im_v = first[RB:]
            pop_i = popcount(i, 5)
            if layer[1] < 0:
                prod = re_v * hats[layer[0], 1, i] - im_v * hats[layer[0], 0, i]
                sums = [None] * 5
                for m in range(16):
                    pop = bin(m).count('1')
                    piece = prod[8 * m:8 * m + 8]
                    sums[pop] = piece if sums[pop] is None else sums[pop] + piece
                flat = sums[0] + sums[1] + sums[2] + sums[3] + sums[4]
                tilt = sums[1] + 2.0 * sums[2] + 3.0 * sums[3] + 4.0 * sums[4]
                weight = wtab[...] - 2.0 * pop_i.astype(F32)
                total = weight * flat - 2.0 * tilt
                acc[1 + layer[0]] += total[:, :LN] + total[:, LN:]
            cos_d = jnp.concatenate([dtab[0, pop_i + bin(m).count('1')] for m in range(16)], axis=0)
            sin_d = jnp.concatenate([dtab[1, pop_i + bin(m).count('1')] for m in range(16)], axis=0)
            re_v, im_v = re_v * cos_d + im_v * sin_d, im_v * cos_d - re_v * sin_d
            if layer[1] > 0:
                hats[layer[0], 0, i] = re_v
                hats[layer[0], 1, i] = im_v
            turned = jnp.concatenate([re_v, im_v], axis=0)
            second = split_dot(turned, had[...])
            for ri in range(2):
                for half in range(2):
                    items = second[RB * ri:RB * ri + RB, LN * half:LN * half + LN]
                    items = butterfly(items.reshape(16, 8, LN), range(4)).reshape(8, 16, LN)
                    for m in range(8):
                        tmp[ri, half, pl.ds(m, 16, stride=8), :] = items[m]
            for ri in range(2):
                for half in range(2):
                    items = butterfly(tmp[ri, half].reshape(16, 8, LN), range(3))
                    work[ri, half, i] = items.reshape(RB, LN)
            return carry

        lax.fori_loop(0, NK, body, 0)

    def last_rows(i):
        for ri in range(2):
            for half in range(2):
                ref = chunk_of(work, ri, half, i)
                radix32(ref, ref)

    def pieces(i, kg):
        return pl.ds(kg * KG, KG), pl.ds(pl.multiple_of(i * CH, CH), CH)

    def mix_pair(own_re, own_im, oth_re, oth_im, cos_b, sin_b):
        return (cos_b * own_re + sin_b * oth_im, cos_b * own_im - sin_b * oth_re,
                cos_b * oth_re + sin_b * own_im, cos_b * oth_im - sin_b * own_re)

    def first_rows(i, received):
        for ri in range(2):
            ref = chunk_of(work, ri, core, i)
            radix32(ref, ref)
            dst = chunk_of(work, ri, other, i)
            radix32(rchunk_of(ri, i) if received else dst, dst)

    for layer in range(3):
        layout = layer % 2
        make_dtab(layer, 1.0)
        sin_b, cos_b = half_angle(layer)
        angle = gamma_ref[pos_y, layer]
        if layer > 0:
            pl.semaphore_wait(credit, 1)

        def send_body(i, carry):
            if layer > 0:
                last_rows(i)

            def point(kg, carry2):
                ks, rows = pieces(i, kg)
                state = []
                for half in range(2):
                    sin_p, cos_p = sincos(angle * cost_half(layout, half, ks, rows))
                    if layer == 0:
                        scale = 2.0 ** (-0.5 * (LOCAL + 1))
                        re_v = cos_p * scale
                        im_v = sin_p * -scale
                    else:
                        re_v = work[0, half, ks, rows, :]
                        im_v = work[1, half, ks, rows, :]
                        re_v, im_v = re_v * cos_p + im_v * sin_p, im_v * cos_p - re_v * sin_p
                        phis[layer - 1, 0, half, ks, rows, :] = re_v
                        phis[layer - 1, 1, half, ks, rows, :] = im_v
                    state += [re_v, im_v]
                state = mix_pair(*state, cos_b, sin_b)
                for half in range(2):
                    for ri in range(2):
                        work[ri, half, ks, rows, :] = state[2 * half + ri]
                return carry2

            lax.fori_loop(0, NK // KG, point, 0)
            exchange(i).start()
            return carry

        lax.fori_loop(0, NCH, send_body, 0)

        def take_body(i, carry):
            exchange(i).wait()
            first_rows(i, True)
            return carry

        lax.fori_loop(0, NCH, take_body, 0)
        pl.semaphore_signal(credit, inc=1, device_id=near_core, device_id_type=MESH)
        inner((layer, 1))

    def turn_body(i, carry):
        last_rows(i)

        def point(kg, total):
            ks, rows = pieces(i, kg)
            for half in range(2):
                cost_v = cost_half(1, half, ks, rows)
                re_v = work[0, half, ks, rows, :]
                im_v = work[1, half, ks, rows, :]
                lam_re = cost_v * re_v
                lam_im = cost_v * im_v
                work[0, half, ks, rows, :] = lam_re
                work[1, half, ks, rows, :] = lam_im
                total = total + jnp.sum(lam_re * re_v + lam_im * im_v, axis=0)
            return total

        acc[0] += lax.fori_loop(0, NK // KG, point, jnp.zeros((CH, LN), F32))
        first_rows(i, False)
        return carry

    lax.fori_loop(0, NCH, turn_body, 0)

    for layer in (2, 1, 0):
        layout = layer % 2
        make_dtab(layer, -1.0)
        sin_b, cos_b = half_angle(layer)
        angle = gamma_ref[pos_y, layer]
        inner((layer, -1))
        pl.semaphore_wait(credit, 1)

        def back_send(i, carry):
            last_rows(i)
            exchange(i).start()
            return carry

        lax.fori_loop(0, NCH, back_send, 0)

        def back_take(i, carry):
            exchange(i).wait()

            def point(kg, sums):
                ks, rows = pieces(i, kg)
                beta_sum, gamma_sum = sums
                own_re = work[0, core, ks, rows, :]
                own_im = work[1, core, ks, rows, :]
                oth_re = recv[0, ks, rows, :]
                oth_im = recv[1, ks, rows, :]
                lam = mix_pair(own_re, own_im, oth_re, oth_im, cos_b, -sin_b)
                lams = {0: lam[:2], 1: lam[2:]}
                phi = []
                costs = []
                waves = []
                for side in (core, other):
                    cost_v = cost_half(layout, side, ks, rows)
                    costs.append(cost_v)
                    sin_p, cos_p = sincos(angle * cost_v)
                    waves.append((sin_p, cos_p))
                    if layer == 0:
                        scale = 2.0 ** (-0.5 * (LOCAL + 1))
                        phi.append((cos_p * scale, sin_p * -scale))
                    else:
                        phi.append((phis[layer - 1, 0, side, ks, rows, :], phis[layer - 1, 1, side, ks, rows, :]))
                for side in range(2):
                    lam_re, lam_im = lams[side]
                    gamma_sum = gamma_sum + jnp.sum(costs[side] * (lam_re * phi[side][1] - lam_im * phi[side][0]), axis=0)
                    beta_sum = beta_sum + jnp.sum(lam_re * phi[1 - side][1] - lam_im * phi[1 - side][0], axis=0)
                    if layer > 0:
                        sin_p, cos_p = waves[side]
                        where = core if side == 0 else other
                        work[0, where, ks, rows, :] = lam_re * cos_p - lam_im * sin_p
                        work[1, where, ks, rows, :] = lam_im * cos_p + lam_re * sin_p
                return beta_sum, gamma_sum

            zero = jnp.zeros((CH, LN), F32)
            beta_sum, gamma_sum = lax.fori_loop(0, NK // KG, point, (zero, zero))
            acc[1 + layer] += beta_sum
            acc[4 + layer] += 2.0 * gamma_sum
            if layer > 0:
                first_rows(i, False)
            return carry

        lax.fori_loop(0, NCH, back_take, 0)
        if layer > 0:
            pl.semaphore_signal(credit, inc=1, device_id=near_core, device_id_type=MESH)

    order = (0, 4, 5, 6, 1, 2, 3)
    rows = [jnp.sum(acc[q], axis=0, keepdims=True) for q in order]
    part[...] = jnp.concatenate(rows + [jnp.zeros((1, LN), F32)], axis=0)
    peers[pos_y, core] = part[...]
    fins = [push(part, peers.at[pos_y, core], fin_s.at[0], fin_r.at[0], near_core),
            push(part, peers.at[pos_y, core], fin_s.at[1], fin_r.at[1], near_y),
            push(part, peers.at[pos_y, core], fin_s.at[2], fin_r.at[2], near_yc)]
    for copy in fins:
        copy.start()
    for copy in fins:
        copy.wait()
    for s in range(2):
        out_ref[s] = jnp.broadcast_to(jnp.sum(peers[s, 0] + peers[s, 1], axis=1, keepdims=True), (8, LN))


def solution(mesh):
    def device_fn(cost, gamma, beta):
        vmem = pl.BlockSpec(memory_space=pltpu.VMEM)
        smem = pl.BlockSpec(memory_space=pltpu.SMEM)
        dma = pltpu.SemaphoreType.DMA
        out = pl.pallas_call(
            kernel,
            out_shape=jax.ShapeDtypeStruct((2, 8, LN), F32),
            in_specs=[vmem, smem, smem],
            out_specs=vmem,
            scratch_shapes=[
                pltpu.VMEM((2, 2, NK, RB, LN), F32),
                pltpu.VMEM((2, 2, NK, RB, LN), F32),
                pltpu.VMEM((2, NK, RB, LN), F32),
                pltpu.VMEM((3, 2, NK, RB, 2 * LN), F32),
                pltpu.VMEM((2, 2, 2, NK, RB, LN), F32),
                pltpu.VMEM((768, 256), BF16),
                pltpu.VMEM((2, 2, RB, LN), F32),
                pltpu.VMEM((2, 10, 8, 256), F32),
                pltpu.VMEM((8, 256), F32),
                pltpu.VMEM((8, 8, LN), F32),
                pltpu.VMEM((8, LN), F32),
                pltpu.VMEM((2, 2, 8, LN), F32),
                dma((2, 4)), dma((2, 4)), dma((4,)), dma((4,)), dma((4, 4)), dma((4, 4)),
                dma((NCH,)), dma((NCH,)), dma((3,)), dma((3,)),
                pltpu.SemaphoreType.REGULAR,
            ],
            compiler_params=pltpu.CompilerParams(collective_id=0, has_side_effects=True, vmem_limit_bytes=67043328),
        )(cost.reshape(16, RB, LN), gamma, beta)
        return out[:, 0, 0], out[:, 1:7, 0]

    cost_spec = P(('inst', 'qy', 'qx'))
    angle_spec = P('inst', None)
    return jax.shard_map(device_fn, mesh=mesh, in_specs=(cost_spec, angle_spec, angle_spec), out_specs=(P('inst'), angle_spec), check_vma=False)
```

```python
import functools
import math
import jax
import jax.numpy as jnp
from jax import lax
from jax.experimental import pallas as pl
from jax.experimental.pallas import tpu as pltpu
from jax.sharding import PartitionSpec as P

F32 = jnp.float32
BF16 = jnp.bfloat16
NK = 32
RB = 128
LN = 128
CH = 8
NCH = RB // CH
GC = 4
KG = 8
MESH = pl.DeviceIdType.MESH
QUBITS = 21
ROWQ = 12


def popcount(value, bits):
    total = value % 2
    for bit in range(1, bits):
        total = total + (value // 2 ** bit) % 2
    return total


def sincos(turns):
    frac = turns - jnp.round(turns)
    sq = frac * frac
    sin_h = 1.098257528e-01
    sin_h = sin_h * sq - 8.461123459e-01
    sin_h = sin_h * sq + 3.606354339e+00
    sin_h = sin_h * sq - 7.308245693e+00
    sin_h = sin_h * sq + 4.442882919e+00
    sin_h = sin_h * frac
    cos_h = -3.450177884e-02
    cos_h = cos_h * sq + 3.322516636e-01
    cos_h = cos_h * sq - 1.888274957e+00
    cos_h = cos_h * sq + 5.739881543e+00
    cos_h = cos_h * sq - 6.978864110e+00
    cos_h = cos_h * sq + 1.414213562e+00
    return sin_h * cos_h, 1.0 - sin_h * sin_h


def butterfly(items, bits):
    shape = items.shape
    for bit in bits:
        step = 1 << bit
        pairs = items.reshape((shape[0] // (2 * step), 2, step) + shape[1:])
        first = pairs[:, 0]
        second = pairs[:, 1]
        items = jnp.stack([first + second, first - second], axis=1).reshape(shape)
    return items


def split(values):
    high = values.astype(BF16)
    rest = values - high.astype(F32)
    mid = rest.astype(BF16)
    return high, mid, (rest - mid.astype(F32)).astype(BF16)


def kernel(cost_ref, gamma_ref, beta_ref, out_ref, cost_all, work, recv, hats, phis, rot, flip, tmp, tmp2, lhs, dtab, wtab, acc, part, peers,
           own_s, own_r, rel_s, rel_r, core_s, core_r, ex_s, ex_r, fin_s, fin_r, credit):
    pos_y = lax.axis_index('qy')
    pos_b = lax.axis_index('qx')
    pos_x = pos_b // 2
    core = pos_b % 2
    other = 1 - core
    near_core = {'qy': pos_y, 'qx': pos_x * 2 + other}
    near_x = {'qy': pos_y, 'qx': (1 - pos_x) * 2 + core}
    near_y = {'qy': 1 - pos_y, 'qx': pos_b}
    near_yc = {'qy': 1 - pos_y, 'qx': pos_x * 2 + other}

    barrier = pltpu.get_barrier_semaphore()
    for dev in (near_core, near_x, near_y, near_yc):
        pl.semaphore_signal(barrier, inc=1, device_id=dev, device_id_type=MESH)
    pl.semaphore_wait(barrier, 4)

    def slot(block_y, block_x, block_core, chunk):
        return cost_all.at[block_y, block_x, pl.ds(block_core * 16 + chunk * GC, GC)]

    def push(src, dst, send, rcv, dev):
        return pltpu.make_async_remote_copy(src_ref=src, dst_ref=dst, send_sem=send, recv_sem=rcv, device_id=dev, device_id_type=MESH)

    sends = []

    def go(copy):
        copy.start()
        sends.append(copy)

    for q in range(4):
        src = cost_ref.at[pl.ds(q * GC, GC)]
        dst = slot(pos_y, pos_x, core, q)
        go(push(src, dst, own_s.at[0, q], own_r.at[0, q], near_x))
        go(push(src, dst, own_s.at[1, q], own_r.at[1, q], near_y))
        go(push(src, dst, core_s.at[0, q], core_r.at[0, q], near_core))

    cost_all[pos_y, pos_x, pl.ds(core * 16, 16)] = cost_ref[...]

    row_i = lax.broadcasted_iota(jnp.int32, (256, 256), 0)
    col_i = lax.broadcasted_iota(jnp.int32, (256, 256), 1)
    differ = row_i ^ col_i
    single = (differ != 0) & ((differ & (differ - 1)) == 0)
    flip_v = jnp.where(single, jnp.where(row_i > col_i, 1.0, -1.0), 0.0).astype(BF16)
    flip[...] = flip_v
    lane_i = lax.broadcasted_iota(jnp.int32, (8, LN), 1)
    sub_i = lax.broadcasted_iota(jnp.int32, (8, LN), 0)
    wtab[...] = (ROWQ - 2 * popcount(sub_i, 3)).astype(F32)
    lane_ones = popcount(lane_i, 7)
    acc[...] = jnp.zeros_like(acc)

    for q in range(4):
        block = slot(pos_y, 1 - pos_x, core, q)
        push(block, block, own_s.at[0, q], own_r.at[0, q], near_x).wait_recv()
        go(push(block, block, core_s.at[1, q], core_r.at[1, q], near_core))
        if q < 2:
            go(push(block, block, rel_s.at[q], rel_r.at[q], near_y))
        block = slot(1 - pos_y, pos_x, core, q)
        push(block, block, own_s.at[1, q], own_r.at[1, q], near_y).wait_recv()
        go(push(block, block, core_s.at[2, q], core_r.at[2, q], near_core))
        if q >= 2:
            go(push(block, block, rel_s.at[q], rel_r.at[q], near_x))
    for q in (0, 2, 1, 3):
        block = slot(1 - pos_y, 1 - pos_x, core, q)
        push(block, block, rel_s.at[q], rel_r.at[q], near_x).wait_recv()
        go(push(block, block, core_s.at[3, q], core_r.at[3, q], near_core))
    for q in range(4):
        for kind, (by, bx) in enumerate(((pos_y, pos_x), (pos_y, 1 - pos_x), (1 - pos_y, pos_x), (1 - pos_y, 1 - pos_x))):
            block = slot(by, bx, other, q)
            push(block, block, core_s.at[kind, q], core_r.at[kind, q], near_core).wait_recv()
    for copy in sends:
        copy.wait_send()

    def make_dtab(layer, sign):
        half = (0.25 / math.pi) * beta_ref[pos_y, layer]
        for pop in range(10):
            sin_v, cos_v = sincos(half * (wtab[...] - 2.0 * pop))
            dtab[0, pop] = cos_v * 2.0 ** -ROWQ
            dtab[1, pop] = sin_v * (sign * 2.0 ** -ROWQ)

    def half_angle(layer):
        return sincos(jnp.full((1, CH, LN), (0.25 / math.pi) * beta_ref[pos_y, layer], F32))

    def make_rot(layer, sign):
        sin_b, cos_b = sincos(jnp.full((8, 256), (0.25 / math.pi) * beta_ref[pos_y, layer], F32))
        sin_b = sin_b * sign
        cols = lax.broadcasted_iota(jnp.int32, (8, 256), 1)

        def body(n, carry):
            tiles = []
            for sub in range(2):
                lines = lax.broadcasted_iota(jnp.int32, (8, 256), 0) + n * 16 + sub * 8
                delta = lines ^ cols
                total = None
                for bit in range(8):
                    factor = jnp.where((delta >> bit) & 1 == 0, cos_b, jnp.where((lines >> bit) & 1 == 1, sin_b, -sin_b))
                    total = factor if total is None else total * factor
                tiles.append(total)
            high, mid, low = split(jnp.concatenate(tiles, axis=0))
            for m, piece in enumerate((high, mid, low)):
                rot[pl.ds(pl.multiple_of(m * 256 + n * 16, 16), 16), :] = piece
            return carry

        lax.fori_loop(0, 16, body, 0)

    def frame(ones):
        turn = ones % 4
        real = jnp.where(turn == 0, 1.0, jnp.where(turn == 2, -1.0, 0.0))
        imag = jnp.where(turn == 1, -1.0, jnp.where(turn == 3, 1.0, 0.0))
        scale = 2.0 ** (-0.5 * QUBITS)
        return real[None] * scale, imag[None] * scale

    def cost_half(layout, half, ks, rows):
        if layout == 0:
            return cost_all[core, half, ks, rows, :]
        return cost_all[half, core, ks, rows, :]

    def radix32(src, dst):
        dst[...] = butterfly(src[...], range(5))

    def chunk_of(ref, ri, half, i):
        return ref.at[ri, half, :, pl.ds(pl.multiple_of(i * CH, CH), CH), :]

    def rchunk_of(ri, i):
        return recv.at[ri, :, pl.ds(pl.multiple_of(i * CH, CH), CH), :]

    def exchange(i):
        rows = pl.ds(pl.multiple_of(i * CH, CH), CH)
        return push(work.at[:, other, :, rows, :], recv.at[:, :, rows, :], ex_s.at[i], ex_r.at[i], near_core)

    def row_wave(i):
        pop_i = popcount(jnp.asarray(i, jnp.int32), 5)
        pops = [bin(m).count('1') for m in range(16)]
        return [jnp.concatenate([dtab[n, pop_i + pop] for pop in pops], axis=0) for n in range(2)]

    def stage_in(i, slot, layer, forward):
        if forward:
            cos_d, sin_d = row_wave(i)
        for half in range(2):
            pair = []
            for ri in range(2):
                items = butterfly(work[ri, half, i].reshape(16, 8, LN), range(3))
                tmp[...] = items.reshape(RB, LN)
                items = [tmp[pl.ds(m, 16, stride=8), :].reshape(1, 2, 8, LN) for m in range(8)]
                pair.append(butterfly(jnp.concatenate(items, axis=0).reshape(16, 8, LN), range(4)).reshape(RB, LN))
            re_v, im_v = pair
            if forward:
                pair = [re_v * cos_d + im_v * sin_d, im_v * cos_d - re_v * sin_d]
            else:
                prod = re_v * hats[layer, 1, half, i] - im_v * hats[layer, 0, half, i]
                sums = [None] * 5
                for m in range(16):
                    pop = bin(m).count('1')
                    piece = prod[8 * m:8 * m + 8]
                    sums[pop] = piece if sums[pop] is None else sums[pop] + piece
                flat = sums[0] + sums[1] + sums[2] + sums[3] + sums[4]
                tilt = sums[1] + 2.0 * sums[2] + 3.0 * sums[3] + 4.0 * sums[4]
                pop_i = popcount(jnp.asarray(i, jnp.int32), 5)
                acc[1 + layer] += (wtab[...] - 2.0 * jnp.asarray(pop_i, F32)) * flat - 2.0 * tilt
            for ri in range(2):
                for n, piece in enumerate(split(pair[ri])):
                    lhs[slot, pl.ds(RB * ri, RB), pl.ds(2 * LN * n + LN * half, LN)] = piece

    def stage_out(i, slot, layer, forward):
        high = lhs[slot, :, 0:256]
        mid = lhs[slot, :, 256:512]
        low = lhs[slot, :, 512:768]
        table = [rot[0:256], rot[256:512], rot[512:768]]
        table = jnp.concatenate([table[0], table[1], table[2], table[0], table[1], table[0]], axis=0)
        prod = jnp.dot(jnp.concatenate([high, high, high, mid, mid, low], axis=1), table, preferred_element_type=F32)
        if not forward:
            turned = jnp.dot(jnp.concatenate([high, mid, low], axis=1), jnp.concatenate([flip[...]] * 3, axis=0), preferred_element_type=F32)
            total = None
            for half in range(2):
                for ri in range(2):
                    piece = turned[RB * ri:RB * ri + RB, LN * half:LN * half + LN] * hats[layer, ri, half, i]
                    piece = jnp.sum(piece.reshape(16, 8, LN), axis=0)
                    total = piece if total is None else total + piece
            acc[1 + layer] -= total
            cos_d, sin_d = row_wave(i)
        for half in range(2):
            re_v = prod[:RB, LN * half:LN * half + LN]
            im_v = prod[RB:, LN * half:LN * half + LN]
            if forward:
                hats[layer, 0, half, i] = re_v
                hats[layer, 1, half, i] = im_v
            else:
                re_v, im_v = re_v * cos_d + im_v * sin_d, im_v * cos_d - re_v * sin_d
            for ri, items in enumerate((re_v, im_v)):
                items = butterfly(items.reshape(16, 8, LN), range(4)).reshape(8, 2, 8, LN)
                for b6 in range(2):
                    tmp2[64 * b6:64 * b6 + 64] = items[:, b6].reshape(64, LN)
                items = [tmp2[pl.ds(m, 16, stride=8), :].reshape(2, 1, 8, LN) for m in range(8)]
                items = butterfly(jnp.concatenate(items, axis=1).reshape(16, 8, LN), range(3))
                work[ri, half, i] = items.reshape(RB, LN)

    def inner(layer, forward):
        stage_in(0, 0, layer, forward)

        def body(p, carry):
            stage_out(p, 0, layer, forward)
            stage_in(p + 1, 0, layer, forward)
            return carry

        lax.fori_loop(0, NK - 1, body, 0)
        stage_out(NK - 1, 0, layer, forward)

    def last_rows(i):
        for ri in range(2):
            for half in range(2):
                ref = chunk_of(work, ri, half, i)
                radix32(ref, ref)

    def pieces(i, kg):
        return pl.ds(kg * KG, KG), pl.ds(pl.multiple_of(i * CH, CH), CH)

    def mix_pair(own_re, own_im, oth_re, oth_im, cos_b, sin_b):
        return (cos_b * own_re + sin_b * oth_re, cos_b * own_im + sin_b * oth_im,
                cos_b * oth_re - sin_b * own_re, cos_b * oth_im - sin_b * own_im)

    def first_rows(i, received):
        for ri in range(2):
            ref = chunk_of(work, ri, core, i)
            radix32(ref, ref)
            dst = chunk_of(work, ri, other, i)
            radix32(rchunk_of(ri, i) if received else dst, dst)

    for layer in range(3):
        layout = layer % 2
        make_dtab(layer, 1.0)
        make_rot(layer, 1.0)
        sin_b, cos_b = half_angle(layer)
        angle = (0.5 / math.pi) * gamma_ref[pos_y, layer]
        if layer > 0:
            pl.semaphore_wait(credit, 1)

        def send_body(i, carry):
            if layer > 0:
                last_rows(i)

            def point(kg, carry2):
                ks, rows = pieces(i, kg)
                state = []
                for half in range(2):
                    sin_p, cos_p = sincos(angle * cost_half(layout, half, ks, rows))
                    if layer == 0:
                        real, imag = frame(lane_ones + core + half)
                        re_v = cos_p * real + sin_p * imag
                        im_v = cos_p * imag - sin_p * real
                    else:
                        re_v = work[0, half, ks, rows, :]
                        im_v = work[1, half, ks, rows, :]
                        re_v, im_v = re_v * cos_p + im_v * sin_p, im_v * cos_p - re_v * sin_p
                        phis[layer - 1, 0, half, ks, rows, :] = re_v
                        phis[layer - 1, 1, half, ks, rows, :] = im_v
                    state += [re_v, im_v]
                state = mix_pair(*state, cos_b, sin_b)
                for half in range(2):
                    for ri in range(2):
                        work[ri, half, ks, rows, :] = state[2 * half + ri]
                return carry2

            lax.fori_loop(0, NK // KG, point, 0)
            exchange(i).start()
            return carry

        lax.fori_loop(0, NCH, send_body, 0)

        def take_body(i, carry):
            exchange(i).wait()
            first_rows(i, True)
            return carry

        lax.fori_loop(0, NCH, take_body, 0)
        pl.semaphore_signal(credit, inc=1, device_id=near_core, device_id_type=MESH)
        inner(layer, True)

    def turn_body(i, carry):
        last_rows(i)

        def point(kg, total):
            ks, rows = pieces(i, kg)
            for half in range(2):
                cost_v = cost_half(1, half, ks, rows)
                re_v = work[0, half, ks, rows, :]
                im_v = work[1, half, ks, rows, :]
                lam_re = cost_v * re_v
                lam_im = cost_v * im_v
                work[0, half, ks, rows, :] = lam_re
                work[1, half, ks, rows, :] = lam_im
                total = total + jnp.sum(lam_re * re_v + lam_im * im_v, axis=0)
            return total

        acc[0] += lax.fori_loop(0, NK // KG, point, jnp.zeros((CH, LN), F32))
        first_rows(i, False)
        return carry

    lax.fori_loop(0, NCH, turn_body, 0)

    for layer in (2, 1, 0):
        layout = layer % 2
        make_dtab(layer, -1.0)
        make_rot(layer, -1.0)
        sin_b, cos_b = half_angle(layer)
        sin_b = sin_b * (2 * core - 1).astype(F32)
        angle = (0.5 / math.pi) * gamma_ref[pos_y, layer]
        inner(layer, False)
        pl.semaphore_wait(credit, 1)

        def back_send(i, carry):
            last_rows(i)
            exchange(i).start()
            return carry

        lax.fori_loop(0, NCH, back_send, 0)

        def back_take(i, carry):
            exchange(i).wait()

            def point(kg, sums):
                ks, rows = pieces(i, kg)
                beta_sum, gamma_sum = sums
                own_re = work[0, core, ks, rows, :]
                own_im = work[1, core, ks, rows, :]
                oth_re = recv[0, ks, rows, :]
                oth_im = recv[1, ks, rows, :]
                lam = mix_pair(own_re, own_im, oth_re, oth_im, cos_b, sin_b)
                lams = {0: lam[:2], 1: lam[2:]}
                phi = []
                costs = []
                waves = []
                for side in (core, other):
                    cost_v = cost_half(layout, side, ks, rows)
                    costs.append(cost_v)
                    sin_p, cos_p = sincos(angle * cost_v)
                    waves.append((sin_p, cos_p))
                    if layer == 0:
                        real, imag = frame(lane_ones + core + side)
                        phi.append((cos_p * real + sin_p * imag, cos_p * imag - sin_p * real))
                    else:
                        phi.append((phis[layer - 1, 0, side, ks, rows, :], phis[layer - 1, 1, side, ks, rows, :]))
                for side in range(2):
                    lam_re, lam_im = lams[side]
                    gamma_sum = gamma_sum + jnp.sum(costs[side] * (lam_re * phi[side][1] - lam_im * phi[side][0]), axis=0)
                    cross = jnp.sum(lam_re * phi[1 - side][0] + lam_im * phi[1 - side][1], axis=0)
                    beta_sum = beta_sum + cross if side == 0 else beta_sum - cross
                    if layer > 0:
                        sin_p, cos_p = waves[side]
                        where = core if side == 0 else other
                        work[0, where, ks, rows, :] = lam_re * cos_p - lam_im * sin_p
                        work[1, where, ks, rows, :] = lam_im * cos_p + lam_re * sin_p
                return beta_sum, gamma_sum

            zero = jnp.zeros((CH, LN), F32)
            beta_sum, gamma_sum = lax.fori_loop(0, NK // KG, point, (zero, zero))
            acc[1 + layer] += beta_sum * (1 - 2 * core).astype(F32)
            acc[4 + layer] += 2.0 * gamma_sum
            if layer > 0:
                first_rows(i, False)
            return carry

        lax.fori_loop(0, NCH, back_take, 0)
        if layer > 0:
            pl.semaphore_signal(credit, inc=1, device_id=near_core, device_id_type=MESH)

    order = (0, 4, 5, 6, 1, 2, 3)
    rows = [jnp.sum(acc[q], axis=0, keepdims=True) for q in order]
    part[...] = jnp.concatenate(rows + [jnp.zeros((1, LN), F32)], axis=0)
    peers[pos_y, core] = part[...]
    fins = [push(part, peers.at[pos_y, core], fin_s.at[0], fin_r.at[0], near_core),
            push(part, peers.at[pos_y, core], fin_s.at[1], fin_r.at[1], near_y),
            push(part, peers.at[pos_y, core], fin_s.at[2], fin_r.at[2], near_yc)]
    for copy in fins:
        copy.start()
    for copy in fins:
        copy.wait()
    for s in range(2):
        out_ref[s] = jnp.broadcast_to(jnp.sum(peers[s, 0] + peers[s, 1], axis=1, keepdims=True), (8, LN))


def solution(mesh):
    def device_fn(cost, gamma, beta):
        vmem = pl.BlockSpec(memory_space=pltpu.VMEM)
        smem = pl.BlockSpec(memory_space=pltpu.SMEM)
        dma = pltpu.SemaphoreType.DMA
        out = pl.pallas_call(
            kernel,
            out_shape=jax.ShapeDtypeStruct((2, 8, LN), F32),
            in_specs=[vmem, smem, smem],
            out_specs=vmem,
            scratch_shapes=[
                pltpu.VMEM((2, 2, NK, RB, LN), F32),
                pltpu.VMEM((2, 2, NK, RB, LN), F32),
                pltpu.VMEM((2, NK, RB, LN), F32),
                pltpu.VMEM((3, 2, 2, NK, RB, LN), F32),
                pltpu.VMEM((2, 2, 2, NK, RB, LN), F32),
                pltpu.VMEM((768, 256), BF16),
                pltpu.VMEM((256, 256), BF16),
                pltpu.VMEM((RB, LN), F32),
                pltpu.VMEM((RB, LN), F32),
                pltpu.VMEM((2, 256, 768), BF16),
                pltpu.VMEM((2, 10, 8, LN), F32),
                pltpu.VMEM((8, LN), F32),
                pltpu.VMEM((8, 8, LN), F32),
                pltpu.VMEM((8, LN), F32),
                pltpu.VMEM((2, 2, 8, LN), F32),
                dma((2, 4)), dma((2, 4)), dma((4,)), dma((4,)), dma((4, 4)), dma((4, 4)),
                dma((NCH,)), dma((NCH,)), dma((3,)), dma((3,)),
                pltpu.SemaphoreType.REGULAR,
            ],
            compiler_params=pltpu.CompilerParams(collective_id=0, has_side_effects=True, vmem_limit_bytes=67043328),
        )(cost.reshape(16, RB, LN), gamma, beta)
        return out[:, 0, 0], out[:, 1:7, 0]

    cost_spec = P(('inst', 'qy', 'qx'))
    angle_spec = P('inst', None)
    return jax.shard_map(device_fn, mesh=mesh, in_specs=(cost_spec, angle_spec, angle_spec), out_specs=(P('inst'), angle_spec), check_vma=False)
```

```python
import functools
import math
import jax
import jax.numpy as jnp
from jax import lax
from jax.experimental import pallas as pl
from jax.experimental.pallas import tpu as pltpu
from jax.sharding import PartitionSpec as P

F32 = jnp.float32
BF16 = jnp.bfloat16
NK = 32
RB = 128
LN = 128
CH = 8
NCH = RB // CH
GC = 4
KG = 8
MESH = pl.DeviceIdType.MESH
QUBITS = 21
ROWQ = 12


def popcount(value, bits):
    total = value % 2
    for bit in range(1, bits):
        total = total + (value // 2 ** bit) % 2
    return total


def sincos(turns):
    frac = turns - jnp.round(turns)
    sq = frac * frac
    sin_h = 1.098257528e-01
    sin_h = sin_h * sq - 8.461123459e-01
    sin_h = sin_h * sq + 3.606354339e+00
    sin_h = sin_h * sq - 7.308245693e+00
    sin_h = sin_h * sq + 4.442882919e+00
    sin_h = sin_h * frac
    cos_h = -3.450177884e-02
    cos_h = cos_h * sq + 3.322516636e-01
    cos_h = cos_h * sq - 1.888274957e+00
    cos_h = cos_h * sq + 5.739881543e+00
    cos_h = cos_h * sq - 6.978864110e+00
    cos_h = cos_h * sq + 1.414213562e+00
    return sin_h * cos_h, 1.0 - sin_h * sin_h


def butterfly(items, bits):
    shape = items.shape
    for bit in bits:
        step = 1 << bit
        pairs = items.reshape((shape[0] // (2 * step), 2, step) + shape[1:])
        first = pairs[:, 0]
        second = pairs[:, 1]
        items = jnp.stack([first + second, first - second], axis=1).reshape(shape)
    return items


def split(values):
    high = values.astype(BF16)
    rest = values - high.astype(F32)
    mid = rest.astype(BF16)
    return high, mid, (rest - mid.astype(F32)).astype(BF16)


def kernel(cost_ref, gamma_ref, beta_ref, out_ref, cost_all, work, recv, hats, phis, waves, rot, flip, tmp, lhs, dtab, wtab, acc, part, peers,
           own_s, own_r, rel_s, rel_r, core_s, core_r, ex_s, ex_r, fin_s, fin_r, credit):
    pos_y = lax.axis_index('qy')
    pos_b = lax.axis_index('qx')
    pos_x = pos_b // 2
    core = pos_b % 2
    other = 1 - core
    near_core = {'qy': pos_y, 'qx': pos_x * 2 + other}
    near_x = {'qy': pos_y, 'qx': (1 - pos_x) * 2 + core}
    near_y = {'qy': 1 - pos_y, 'qx': pos_b}
    others = []
    for d in range(1, 8):
        to_y = 1 - pos_y if d & 4 else pos_y
        to_x = 1 - pos_x if d & 2 else pos_x
        to_core = other if d & 1 else core
        others.append({'qy': to_y, 'qx': to_x * 2 + to_core})

    barrier = pltpu.get_barrier_semaphore()
    for dev in others:
        pl.semaphore_signal(barrier, inc=1, device_id=dev, device_id_type=MESH)
    pl.semaphore_wait(barrier, 7)

    def slot(block_y, block_x, block_core, chunk):
        return cost_all.at[block_y, block_x, pl.ds(block_core * 16 + chunk * GC, GC)]

    def push(src, dst, send, rcv, dev):
        return pltpu.make_async_remote_copy(src_ref=src, dst_ref=dst, send_sem=send, recv_sem=rcv, device_id=dev, device_id_type=MESH)

    sends = []

    def go(copy):
        copy.start()
        sends.append(copy)

    for q in range(4):
        src = cost_ref.at[pl.ds(q * GC, GC)]
        dst = slot(pos_y, pos_x, core, q)
        go(push(src, dst, own_s.at[0, q], own_r.at[0, q], near_x))
        go(push(src, dst, own_s.at[1, q], own_r.at[1, q], near_y))
        go(push(src, dst, core_s.at[0, q], core_r.at[0, q], near_core))

    cost_all[pos_y, pos_x, pl.ds(core * 16, 16)] = cost_ref[...]

    row_i = lax.broadcasted_iota(jnp.int32, (256, 256), 0)
    col_i = lax.broadcasted_iota(jnp.int32, (256, 256), 1)
    differ = row_i ^ col_i
    single = (differ != 0) & ((differ & (differ - 1)) == 0)
    flip_v = jnp.where(single, jnp.where(row_i > col_i, 1.0, -1.0), 0.0).astype(BF16)
    flip[...] = flip_v
    lane_i = lax.broadcasted_iota(jnp.int32, (8, LN), 1)
    sub_i = lax.broadcasted_iota(jnp.int32, (8, LN), 0)
    wtab[...] = (ROWQ - 2 * popcount(sub_i, 3)).astype(F32)
    lane_ones = popcount(lane_i, 7)
    acc[...] = jnp.zeros_like(acc)

    for q in range(4):
        block = slot(pos_y, 1 - pos_x, core, q)
        push(block, block, own_s.at[0, q], own_r.at[0, q], near_x).wait_recv()
        go(push(block, block, core_s.at[1, q], core_r.at[1, q], near_core))
        if q < 2:
            go(push(block, block, rel_s.at[q], rel_r.at[q], near_y))
        block = slot(1 - pos_y, pos_x, core, q)
        push(block, block, own_s.at[1, q], own_r.at[1, q], near_y).wait_recv()
        go(push(block, block, core_s.at[2, q], core_r.at[2, q], near_core))
        if q >= 2:
            go(push(block, block, rel_s.at[q], rel_r.at[q], near_x))
    for q in (0, 2, 1, 3):
        block = slot(1 - pos_y, 1 - pos_x, core, q)
        push(block, block, rel_s.at[q], rel_r.at[q], near_x).wait_recv()
        go(push(block, block, core_s.at[3, q], core_r.at[3, q], near_core))
    for q in range(4):
        for kind, (by, bx) in enumerate(((pos_y, pos_x), (pos_y, 1 - pos_x), (1 - pos_y, pos_x), (1 - pos_y, 1 - pos_x))):
            block = slot(by, bx, other, q)
            push(block, block, core_s.at[kind, q], core_r.at[kind, q], near_core).wait_recv()
    for copy in sends:
        copy.wait_send()

    def make_dtab(layer, sign):
        half = (0.25 / math.pi) * beta_ref[pos_y, layer]
        for pop in range(10):
            sin_v, cos_v = sincos(half * (wtab[...] - 2.0 * pop))
            dtab[0, pop] = cos_v * 2.0 ** -ROWQ
            dtab[1, pop] = sin_v * (sign * 2.0 ** -ROWQ)

    def half_angle(layer):
        return sincos(jnp.full((1, CH, LN), (0.25 / math.pi) * beta_ref[pos_y, layer], F32))

    def make_rot(layer, sign):
        sin_b, cos_b = sincos(jnp.full((8, 256), (0.25 / math.pi) * beta_ref[pos_y, layer], F32))
        sin_b = sin_b * sign
        cols = lax.broadcasted_iota(jnp.int32, (8, 256), 1)

        def body(n, carry):
            tiles = []
            for sub in range(2):
                lines = lax.broadcasted_iota(jnp.int32, (8, 256), 0) + n * 16 + sub * 8
                delta = lines ^ cols
                total = None
                for bit in range(8):
                    factor = jnp.where((delta >> bit) & 1 == 0, cos_b, jnp.where((lines >> bit) & 1 == 1, sin_b, -sin_b))
                    total = factor if total is None else total * factor
                tiles.append(total)
            high, mid, low = split(jnp.concatenate(tiles, axis=0))
            for m, piece in enumerate((high, mid, low)):
                rot[pl.ds(pl.multiple_of(m * 256 + n * 16, 16), 16), :] = piece
            return carry

        lax.fori_loop(0, 16, body, 0)

    def frame(ones):
        turn = ones % 4
        real = jnp.where(turn == 0, 1.0, jnp.where(turn == 2, -1.0, 0.0))
        imag = jnp.where(turn == 1, -1.0, jnp.where(turn == 3, 1.0, 0.0))
        scale = 2.0 ** (-0.5 * QUBITS)
        return real[None] * scale, imag[None] * scale

    def cost_half(layout, half, ks, rows):
        return cost_all[(1 - layout) * core + layout * half, (1 - layout) * half + layout * core, ks, rows, :]

    def radix32(src, dst):
        dst[...] = butterfly(src[...], range(5))

    def chunk_of(ref, ri, half, i):
        return ref.at[ri, half, :, pl.ds(pl.multiple_of(i * CH, CH), CH), :]

    def rchunk_of(ri, i):
        return recv.at[ri, :, pl.ds(pl.multiple_of(i * CH, CH), CH), :]

    def exchange(i):
        rows = pl.ds(pl.multiple_of(i * CH, CH), CH)
        return push(work.at[:, other, :, rows, :], recv.at[:, :, rows, :], ex_s.at[i], ex_r.at[i], near_core)

    def row_wave(i):
        pop_i = popcount(jnp.asarray(i, jnp.int32), 5)
        pops = [bin(m).count('1') for m in range(16)]
        return [jnp.concatenate([dtab[n, pop_i + pop] for pop in pops], axis=0) for n in range(2)]

    def stage_in(i, slot, layer, forward, mine):
        t = i - 16 * pos_x
        if forward:
            cos_d, sin_d = row_wave(i)
        for half in range(2):
            pair = []
            for ri in range(2):
                items = butterfly(work[ri, half, i].reshape(16, 8, LN), range(3))
                tmp[...] = items.reshape(RB, LN)
                items = [tmp[pl.ds(m, 16, stride=8), :].reshape(1, 2, 8, LN) for m in range(8)]
                pair.append(butterfly(jnp.concatenate(items, axis=0).reshape(16, 8, LN), range(4)).reshape(RB, LN))
            re_v, im_v = pair
            if forward:
                pair = [re_v * cos_d + im_v * sin_d, im_v * cos_d - re_v * sin_d]
            elif mine:
                prod = re_v * hats[layer, 1, half, t] - im_v * hats[layer, 0, half, t]
                sums = [None] * 5
                for m in range(16):
                    pop = bin(m).count('1')
                    piece = prod[8 * m:8 * m + 8]
                    sums[pop] = piece if sums[pop] is None else sums[pop] + piece
                flat = sums[0] + sums[1] + sums[2] + sums[3] + sums[4]
                tilt = sums[1] + 2.0 * sums[2] + 3.0 * sums[3] + 4.0 * sums[4]
                pop_i = popcount(jnp.asarray(i, jnp.int32), 5)
                acc[1 + layer] += (wtab[...] - 2.0 * jnp.asarray(pop_i, F32)) * flat - 2.0 * tilt
            for ri in range(2):
                for n, piece in enumerate(split(pair[ri])):
                    lhs[slot, pl.ds(RB * ri, RB), pl.ds(2 * LN * n + LN * half, LN)] = piece

    def stage_mm(i, slot, layer, forward, mine):
        t = i - 16 * pos_x
        high = lhs[slot, :, 0:256]
        mid = lhs[slot, :, 256:512]
        low = lhs[slot, :, 512:768]
        table = [rot[0:256], rot[256:512], rot[512:768]]
        table = jnp.concatenate([table[0], table[1], table[2], table[0], table[1], table[0]], axis=0)
        prod = jnp.dot(jnp.concatenate([high, high, high, mid, mid, low], axis=1), table, preferred_element_type=F32)
        if not forward and mine:
            turned = jnp.dot(jnp.concatenate([high, mid, low], axis=1), jnp.concatenate([flip[...]] * 3, axis=0), preferred_element_type=F32)
            total = None
            for half in range(2):
                for ri in range(2):
                    piece = turned[RB * ri:RB * ri + RB, LN * half:LN * half + LN] * hats[layer, ri, half, t]
                    piece = jnp.sum(piece.reshape(16, 8, LN), axis=0)
                    total = piece if total is None else total + piece
            acc[1 + layer] -= total
        return prod

    def stage_out(prod, i, layer, forward, mine):
        t = i - 16 * pos_x
        if not forward:
            cos_d, sin_d = row_wave(i)
        for half in range(2):
            re_v = prod[:RB, LN * half:LN * half + LN]
            im_v = prod[RB:, LN * half:LN * half + LN]
            if forward and mine:
                hats[layer, 0, half, t] = re_v
                hats[layer, 1, half, t] = im_v
            if not forward:
                re_v, im_v = re_v * cos_d + im_v * sin_d, im_v * cos_d - re_v * sin_d
            for ri, items in enumerate((re_v, im_v)):
                items = butterfly(items.reshape(16, 8, LN), range(4)).reshape(8, 2, 8, LN)
                for b6 in range(2):
                    tmp[64 * b6:64 * b6 + 64] = items[:, b6].reshape(64, LN)
                items = [tmp[pl.ds(m, 16, stride=8), :].reshape(2, 1, 8, LN) for m in range(8)]
                items = butterfly(jnp.concatenate(items, axis=1).reshape(16, 8, LN), range(3))
                work[ri, half, i] = items.reshape(RB, LN)

    def inner(layer, forward):
        def body(mine):
            def both(i, slot):
                prod = stage_mm(i, slot, layer, forward, mine)
                stage_in(i + 1, 1 - slot, layer, forward, mine)
                stage_out(prod, i, layer, forward, mine)

            def two(p, carry):
                i = start + 2 * p
                both(i, 0)
                both(i + 1, 1)
                return carry
            start = first if mine else second
            lax.fori_loop(0, 7, two, 0)
            both(start + 14, 0)

        first = 16 * pos_x
        second = 16 - first
        stage_in(first, 0, layer, forward, True)
        body(True)
        prod = stage_mm(first + 15, 1, layer, forward, True)
        stage_in(second, 0, layer, forward, False)
        stage_out(prod, first + 15, layer, forward, True)
        body(False)
        stage_out(stage_mm(second + 15, 1, layer, forward, False), second + 15, layer, forward, False)

    def last_rows(i):
        for ri in range(2):
            for half in range(2):
                ref = chunk_of(work, ri, half, i)
                radix32(ref, ref)

    def pieces(i, kg):
        return pl.ds(kg * KG, KG), pl.ds(pl.multiple_of(i * CH, CH), CH)

    def mix_pair(own_re, own_im, oth_re, oth_im, cos_b, sin_b):
        return (cos_b * own_re + sin_b * oth_re, cos_b * own_im + sin_b * oth_im,
                cos_b * oth_re - sin_b * own_re, cos_b * oth_im - sin_b * own_im)

    def first_rows(i, received):
        for ri in range(2):
            ref = chunk_of(work, ri, core, i)
            radix32(ref, ref)
            dst = chunk_of(work, ri, other, i)
            radix32(rchunk_of(ri, i) if received else dst, dst)

    def give_credit():
        pl.semaphore_signal(credit, inc=1, device_id=near_core, device_id_type=MESH)

    give_credit()

    def send_layer(layer, initial, sin_b, cos_b):
        layout = layer % 2
        angle = (0.5 / math.pi) * gamma_ref[pos_y, layer]

        def send_body(mine):
            def one(n, carry):
                i = (n + 8 * pos_x) % NCH
                if not initial:
                    last_rows(i)

                def point(kg, carry2):
                    ks, rows = pieces(i, kg)
                    here = pieces(n, kg)[1]
                    state = []
                    for half in range(2):
                        sin_p, cos_p = sincos(angle * cost_half(layout, half, ks, rows))
                        if initial:
                            real, imag = frame(lane_ones + core + half)
                            re_v = cos_p * real + sin_p * imag
                            im_v = cos_p * imag - sin_p * real
                        else:
                            re_v = work[0, half, ks, rows, :]
                            im_v = work[1, half, ks, rows, :]
                            re_v, im_v = re_v * cos_p + im_v * sin_p, im_v * cos_p - re_v * sin_p
                            waves[layer - 1, 0, half, ks, rows, :] = cos_p
                            waves[layer - 1, 1, half, ks, rows, :] = sin_p
                            if mine:
                                phis[layer - 1, 0, half, ks, here, :] = re_v
                                phis[layer - 1, 1, half, ks, here, :] = im_v
                        state += [re_v, im_v]
                    state = mix_pair(*state, cos_b, sin_b)
                    for half in range(2):
                        for ri in range(2):
                            work[ri, half, ks, rows, :] = state[2 * half + ri]
                    return carry2

                lax.fori_loop(0, NK // KG, point, 0)
                exchange(i).start()
                return carry
            return one

        lax.fori_loop(0, NCH // 2, send_body(True), 0)
        lax.fori_loop(NCH // 2, NCH, send_body(False), 0)

    def forward_layer(layer, carry):
        make_dtab(layer, 1.0)
        make_rot(layer, 1.0)
        sin_b, cos_b = half_angle(layer)
        pl.semaphore_wait(credit, 1)

        @pl.when(layer == 0)
        def _():
            send_layer(layer, True, sin_b, cos_b)

        @pl.when(layer > 0)
        def _():
            send_layer(layer, False, sin_b, cos_b)

        def take_body(n, carry2):
            i = (n + 8 * pos_x) % NCH
            exchange(i).wait()
            first_rows(i, True)
            return carry2

        lax.fori_loop(0, NCH, take_body, 0)
        give_credit()
        inner(layer, True)
        return carry

    lax.fori_loop(0, 3, forward_layer, 0)

    def turn_body(i, carry):
        total = jnp.zeros((CH, LN), F32)
        for half in range(2):
            for ri in range(2):
                ref = chunk_of(work, ri, half, i)
                values = butterfly(ref[...], range(5))
                lam = values * cost_half(1, half, slice(None), pl.ds(pl.multiple_of(i * CH, CH), CH))
                total = total + jnp.sum(values * lam, axis=0)
                ref[...] = butterfly(lam, range(5))
        acc[0] += 0.5 * total
        return carry

    lax.fori_loop(0, NCH, turn_body, 0)

    def backward_layer(back, carry0):
        layer = 2 - back
        layout = layer % 2
        make_dtab(layer, -1.0)
        make_rot(layer, -1.0)
        sin_b, cos_b = half_angle(layer)
        sin_b = sin_b * (2 * core - 1).astype(F32)
        angle = (0.5 / math.pi) * gamma_ref[pos_y, layer]
        inner(layer, False)
        pl.semaphore_wait(credit, 1)
        count = NCH // 2 + (NCH // 2) * ((layer + 1) // 2)

        def back_send(n, carry):
            i = (n + 8 * pos_x) % NCH
            last_rows(i)
            exchange(i).start()
            return carry

        lax.fori_loop(0, count, back_send, 0)

        def back_take(mine, final):
            def one(n, carry):
                i = (n + 8 * pos_x) % NCH
                exchange(i).wait()

                def point(kg, sums):
                    ks, rows = pieces(i, kg)
                    here = pieces(n, kg)[1]
                    beta_sum, gamma_sum = sums
                    own_re = work[0, core, ks, rows, :]
                    own_im = work[1, core, ks, rows, :]
                    oth_re = recv[0, ks, rows, :]
                    oth_im = recv[1, ks, rows, :]
                    lam = mix_pair(own_re, own_im, oth_re, oth_im, cos_b, sin_b)
                    lams = (lam[:2], lam[2:])
                    if mine:
                        phi = []
                        costs = []
                        for side in (core, other):
                            cost_v = cost_half(layout, side, ks, rows)
                            costs.append(cost_v)
                            if final:
                                sin_p, cos_p = sincos(angle * cost_v)
                                real, imag = frame(lane_ones + core + side)
                                phi.append((cos_p * real + sin_p * imag, cos_p * imag - sin_p * real))
                            else:
                                phi.append((phis[layer - 1, 0, side, ks, here, :], phis[layer - 1, 1, side, ks, here, :]))
                        for side in range(2):
                            lam_re, lam_im = lams[side]
                            gamma_sum = gamma_sum + jnp.sum(costs[side] * (lam_re * phi[side][1] - lam_im * phi[side][0]), axis=0)
                            cross = jnp.sum(lam_re * phi[1 - side][0] + lam_im * phi[1 - side][1], axis=0)
                            beta_sum = beta_sum + cross if side == 0 else beta_sum - cross
                    if not final:
                        for side, where in enumerate((core, other)):
                            lam_re, lam_im = lams[side]
                            cos_p = waves[layer - 1, 0, where, ks, rows, :]
                            sin_p = waves[layer - 1, 1, where, ks, rows, :]
                            work[0, where, ks, rows, :] = lam_re * cos_p - lam_im * sin_p
                            work[1, where, ks, rows, :] = lam_im * cos_p + lam_re * sin_p
                    return beta_sum, gamma_sum

                zero = jnp.zeros((CH, LN), F32)
                beta_sum, gamma_sum = lax.fori_loop(0, NK // KG, point, (zero, zero))
                if mine:
                    acc[1 + layer] += beta_sum * (1 - 2 * core).astype(F32)
                    acc[4 + layer] += 2.0 * gamma_sum
                if not final:
                    first_rows(i, False)
                return carry
            return one

        @pl.when(layer > 0)
        def _():
            lax.fori_loop(0, NCH // 2, back_take(True, False), 0)
            lax.fori_loop(NCH // 2, NCH, back_take(False, False), 0)

        @pl.when(layer == 0)
        def _():
            lax.fori_loop(0, NCH // 2, back_take(True, True), 0)

        give_credit()
        return carry0

    lax.fori_loop(0, 3, backward_layer, 0)
    pl.semaphore_wait(credit, 1)

    order = (0, 4, 5, 6, 1, 2, 3)
    rows = [jnp.sum(acc[q], axis=0, keepdims=True) for q in order]
    part[...] = jnp.concatenate(rows + [jnp.zeros((1, LN), F32)], axis=0)
    peers[pos_y, pos_b] = part[...]
    fins = [push(part, peers.at[pos_y, pos_b], fin_s.at[n], fin_r.at[n], dev) for n, dev in enumerate(others)]
    for copy in fins:
        copy.start()
    for copy in fins:
        copy.wait()
    for n in range(2):
        total = peers[n, 0] + peers[n, 1] + peers[n, 2] + peers[n, 3]
        out_ref[n] = jnp.broadcast_to(jnp.sum(total, axis=1, keepdims=True), (8, LN))


def solution(mesh):
    def device_fn(cost, gamma, beta):
        vmem = pl.BlockSpec(memory_space=pltpu.VMEM)
        smem = pl.BlockSpec(memory_space=pltpu.SMEM)
        dma = pltpu.SemaphoreType.DMA
        out = pl.pallas_call(
            kernel,
            out_shape=jax.ShapeDtypeStruct((2, 8, LN), F32),
            in_specs=[vmem, smem, smem],
            out_specs=vmem,
            scratch_shapes=[
                pltpu.VMEM((2, 2, NK, RB, LN), F32),
                pltpu.VMEM((2, 2, NK, RB, LN), F32),
                pltpu.VMEM((2, NK, RB, LN), F32),
                pltpu.VMEM((3, 2, 2, NK // 2, RB, LN), F32),
                pltpu.VMEM((2, 2, 2, NK, RB // 2, LN), F32),
                pltpu.VMEM((2, 2, 2, NK, RB, LN), F32),
                pltpu.VMEM((768, 256), BF16),
                pltpu.VMEM((256, 256), BF16),
                pltpu.VMEM((RB, LN), F32),
                pltpu.VMEM((2, 256, 768), BF16),
                pltpu.VMEM((2, 10, 8, LN), F32),
                pltpu.VMEM((8, LN), F32),
                pltpu.VMEM((8, 8, LN), F32),
                pltpu.VMEM((8, LN), F32),
                pltpu.VMEM((2, 4, 8, LN), F32),
                dma((2, 4)), dma((2, 4)), dma((4,)), dma((4,)), dma((4, 4)), dma((4, 4)),
                dma((NCH,)), dma((NCH,)), dma((7,)), dma((7,)),
                pltpu.SemaphoreType.REGULAR,
            ],
            compiler_params=pltpu.CompilerParams(collective_id=0, has_side_effects=True, vmem_limit_bytes=67043328),
        )(cost.reshape(16, RB, LN), gamma, beta)
        return out[:, 0, 0], out[:, 1:7, 0]

    cost_spec = P(('inst', 'qy', 'qx'))
    angle_spec = P('inst', None)
    return jax.shard_map(device_fn, mesh=mesh, in_specs=(cost_spec, angle_spec, angle_spec), out_specs=(P('inst'), angle_spec), check_vma=False)
```

```python
import functools
import math
import jax
import jax.numpy as jnp
from jax import lax
from jax.experimental import pallas as pl
from jax.experimental.pallas import tpu as pltpu
from jax.sharding import PartitionSpec as P

F32 = jnp.float32
BF16 = jnp.bfloat16
NK = 32
RB = 128
LN = 128
CH = 8
NCH = RB // CH
GC = 4
KG = 8
MESH = pl.DeviceIdType.MESH
QUBITS = 21
ROWQ = 12


def popcount(value, bits):
    total = value % 2
    for bit in range(1, bits):
        total = total + (value // 2 ** bit) % 2
    return total


def sincos(turns):
    frac = turns - jnp.round(turns)
    sq = frac * frac
    sin_h = 1.098257528e-01
    sin_h = sin_h * sq - 8.461123459e-01
    sin_h = sin_h * sq + 3.606354339e+00
    sin_h = sin_h * sq - 7.308245693e+00
    sin_h = sin_h * sq + 4.442882919e+00
    sin_h = sin_h * frac
    cos_h = -3.450177884e-02
    cos_h = cos_h * sq + 3.322516636e-01
    cos_h = cos_h * sq - 1.888274957e+00
    cos_h = cos_h * sq + 5.739881543e+00
    cos_h = cos_h * sq - 6.978864110e+00
    cos_h = cos_h * sq + 1.414213562e+00
    return sin_h * cos_h, 1.0 - sin_h * sin_h


def butterfly(items, bits):
    shape = items.shape
    for bit in bits:
        step = 1 << bit
        pairs = items.reshape((shape[0] // (2 * step), 2, step) + shape[1:])
        first = pairs[:, 0]
        second = pairs[:, 1]
        items = jnp.stack([first + second, first - second], axis=1).reshape(shape)
    return items


def split(values):
    high = values.astype(BF16)
    rest = values - high.astype(F32)
    mid = rest.astype(BF16)
    return high, mid, (rest - mid.astype(F32)).astype(BF16)


def kernel(cost_ref, gamma_ref, beta_ref, energy_ref, grad_ref, cost_all, work, recv, hats, phis, waves, rot, flip, tmp, lhs, dtab, wtab, acc, part, peers,
           own_s, own_r, rel_s, rel_r, core_s, core_r, ex_s, ex_r, fin_s, fin_r, credit):
    pos_y = lax.axis_index('qy')
    pos_b = lax.axis_index('qx')
    pos_x = pos_b // 2
    core = pos_b % 2
    other = 1 - core
    near_core = {'qy': pos_y, 'qx': pos_x * 2 + other}
    near_x = {'qy': pos_y, 'qx': (1 - pos_x) * 2 + core}
    near_y = {'qy': 1 - pos_y, 'qx': pos_b}
    others = []
    for d in range(1, 8):
        to_y = 1 - pos_y if d & 4 else pos_y
        to_x = 1 - pos_x if d & 2 else pos_x
        to_core = other if d & 1 else core
        others.append({'qy': to_y, 'qx': to_x * 2 + to_core})

    barrier = pltpu.get_barrier_semaphore()
    for dev in others:
        pl.semaphore_signal(barrier, inc=1, device_id=dev, device_id_type=MESH)
    pl.semaphore_wait(barrier, 7)

    def slot(block_y, block_x, block_core, chunk):
        return cost_all.at[block_y, block_x, pl.ds(block_core * 16 + chunk * GC, GC)]

    def push(src, dst, send, rcv, dev):
        return pltpu.make_async_remote_copy(src_ref=src, dst_ref=dst, send_sem=send, recv_sem=rcv, device_id=dev, device_id_type=MESH)

    sends = []

    def go(copy):
        copy.start()
        sends.append(copy)

    for q in range(4):
        src = cost_ref.at[pl.ds(q * GC, GC)]
        dst = slot(pos_y, pos_x, core, q)
        go(push(src, dst, own_s.at[0, q], own_r.at[0, q], near_x))
        go(push(src, dst, own_s.at[1, q], own_r.at[1, q], near_y))
        go(push(src, dst, core_s.at[0, q], core_r.at[0, q], near_core))

    cost_all[pos_y, pos_x, pl.ds(core * 16, 16)] = cost_ref[...]

    row_i = lax.broadcasted_iota(jnp.int32, (256, 256), 0)
    col_i = lax.broadcasted_iota(jnp.int32, (256, 256), 1)
    differ = row_i ^ col_i
    single = (differ != 0) & ((differ & (differ - 1)) == 0)
    flip_v = jnp.where(single, jnp.where(row_i > col_i, 1.0, -1.0), 0.0).astype(BF16)
    flip[...] = flip_v
    lane_i = lax.broadcasted_iota(jnp.int32, (8, LN), 1)
    sub_i = lax.broadcasted_iota(jnp.int32, (8, LN), 0)
    wtab[...] = (ROWQ - 2 * popcount(sub_i, 3)).astype(F32)
    lane_ones = popcount(lane_i, 7)
    acc[...] = jnp.zeros_like(acc)

    for q in range(4):
        block = slot(pos_y, 1 - pos_x, core, q)
        push(block, block, own_s.at[0, q], own_r.at[0, q], near_x).wait_recv()
        go(push(block, block, core_s.at[1, q], core_r.at[1, q], near_core))
        if q < 2:
            go(push(block, block, rel_s.at[q], rel_r.at[q], near_y))
        block = slot(1 - pos_y, pos_x, core, q)
        push(block, block, own_s.at[1, q], own_r.at[1, q], near_y).wait_recv()
        go(push(block, block, core_s.at[2, q], core_r.at[2, q], near_core))
        if q >= 2:
            go(push(block, block, rel_s.at[q], rel_r.at[q], near_x))
    for q in (0, 2, 1, 3):
        block = slot(1 - pos_y, 1 - pos_x, core, q)
        push(block, block, rel_s.at[q], rel_r.at[q], near_x).wait_recv()
        go(push(block, block, core_s.at[3, q], core_r.at[3, q], near_core))
    for q in range(4):
        for kind, (by, bx) in enumerate(((pos_y, pos_x), (pos_y, 1 - pos_x), (1 - pos_y, pos_x), (1 - pos_y, 1 - pos_x))):
            block = slot(by, bx, other, q)
            push(block, block, core_s.at[kind, q], core_r.at[kind, q], near_core).wait_recv()
    for copy in sends:
        copy.wait_send()

    def make_dtab(layer, sign):
        half = (0.25 / math.pi) * beta_ref[pos_y, layer]
        for pop in range(10):
            sin_v, cos_v = sincos(half * (wtab[...] - 2.0 * pop))
            dtab[0, pop] = cos_v * 2.0 ** -ROWQ
            dtab[1, pop] = sin_v * (sign * 2.0 ** -ROWQ)

    def half_angle(layer):
        return sincos(jnp.full((1, CH, LN), (0.25 / math.pi) * beta_ref[pos_y, layer], F32))

    def make_rot(layer, sign):
        sin_b, cos_b = sincos(jnp.full((8, 256), (0.25 / math.pi) * beta_ref[pos_y, layer], F32))
        sin_b = sin_b * sign
        cols = lax.broadcasted_iota(jnp.int32, (8, 256), 1)

        def body(n, carry):
            tiles = []
            for sub in range(2):
                lines = lax.broadcasted_iota(jnp.int32, (8, 256), 0) + n * 16 + sub * 8
                delta = lines ^ cols
                total = None
                for bit in range(8):
                    factor = jnp.where((delta >> bit) & 1 == 0, cos_b, jnp.where((lines >> bit) & 1 == 1, sin_b, -sin_b))
                    total = factor if total is None else total * factor
                tiles.append(total)
            high, mid, low = split(jnp.concatenate(tiles, axis=0))
            for m, piece in enumerate((high, mid, low)):
                rot[pl.ds(pl.multiple_of(m * 256 + n * 16, 16), 16), :] = piece
            return carry

        lax.fori_loop(0, 16, body, 0)

    def frame(ones):
        turn = ones % 4
        real = jnp.where(turn == 0, 1.0, jnp.where(turn == 2, -1.0, 0.0))
        imag = jnp.where(turn == 1, -1.0, jnp.where(turn == 3, 1.0, 0.0))
        scale = 2.0 ** (-0.5 * QUBITS)
        return real[None] * scale, imag[None] * scale

    def cost_half(layout, half, ks, rows):
        return cost_all[(1 - layout) * core + layout * half, (1 - layout) * half + layout * core, ks, rows, :]

    def radix32(src, dst):
        dst[...] = butterfly(src[...], range(5))

    def chunk_of(ref, ri, half, i):
        return ref.at[ri, half, :, pl.ds(pl.multiple_of(i * CH, CH), CH), :]

    def rchunk_of(ri, i):
        return recv.at[ri, :, pl.ds(pl.multiple_of(i * CH, CH), CH), :]

    def exchange(i):
        rows = pl.ds(pl.multiple_of(i * CH, CH), CH)
        return push(work.at[:, other, :, rows, :], recv.at[:, :, rows, :], ex_s.at[i], ex_r.at[i], near_core)

    def row_wave(i):
        pop_i = popcount(jnp.asarray(i, jnp.int32), 5)
        pops = [bin(m).count('1') for m in range(16)]
        return [jnp.concatenate([dtab[n, pop_i + pop] for pop in pops], axis=0) for n in range(2)]

    def stage_in(i, slot, layer, forward, mine):
        t = i - 16 * pos_x
        if forward:
            cos_d, sin_d = row_wave(i)
        for half in range(2):
            pair = []
            for ri in range(2):
                items = butterfly(work[ri, half, i].reshape(16, 8, LN), range(3))
                tmp[...] = items.reshape(RB, LN)
                items = [tmp[pl.ds(m, 16, stride=8), :].reshape(1, 2, 8, LN) for m in range(8)]
                pair.append(butterfly(jnp.concatenate(items, axis=0).reshape(16, 8, LN), range(4)).reshape(RB, LN))
            re_v, im_v = pair
            if forward:
                pair = [re_v * cos_d + im_v * sin_d, im_v * cos_d - re_v * sin_d]
            elif mine:
                prod = re_v * hats[layer, 1, half, t] - im_v * hats[layer, 0, half, t]
                sums = [None] * 5
                for m in range(16):
                    pop = bin(m).count('1')
                    piece = prod[8 * m:8 * m + 8]
                    sums[pop] = piece if sums[pop] is None else sums[pop] + piece
                flat = sums[0] + sums[1] + sums[2] + sums[3] + sums[4]
                tilt = sums[1] + 2.0 * sums[2] + 3.0 * sums[3] + 4.0 * sums[4]
                pop_i = popcount(jnp.asarray(i, jnp.int32), 5)
                acc[1 + layer] += (wtab[...] - 2.0 * jnp.asarray(pop_i, F32)) * flat - 2.0 * tilt
            for ri in range(2):
                for n, piece in enumerate(split(pair[ri])):
                    lhs[slot, pl.ds(RB * ri, RB), pl.ds(2 * LN * n + LN * half, LN)] = piece

    def stage_mm(i, slot, layer, forward, mine):
        t = i - 16 * pos_x
        high = lhs[slot, :, 0:256]
        mid = lhs[slot, :, 256:512]
        low = lhs[slot, :, 512:768]
        table = [rot[0:256], rot[256:512], rot[512:768]]
        table = jnp.concatenate([table[0], table[1], table[2], table[0], table[1], table[0]], axis=0)
        prod = jnp.dot(jnp.concatenate([high, high, high, mid, mid, low], axis=1), table, preferred_element_type=F32)
        if not forward and mine:
            turned = jnp.dot(jnp.concatenate([high, mid, low], axis=1), jnp.concatenate([flip[...]] * 3, axis=0), preferred_element_type=F32)
            total = None
            for half in range(2):
                for ri in range(2):
                    piece = turned[RB * ri:RB * ri + RB, LN * half:LN * half + LN] * hats[layer, ri, half, t]
                    piece = jnp.sum(piece.reshape(16, 8, LN), axis=0)
                    total = piece if total is None else total + piece
            acc[1 + layer] -= total
        return prod

    def stage_out(prod, i, layer, forward, mine):
        t = i - 16 * pos_x
        if not forward:
            cos_d, sin_d = row_wave(i)
        for half in range(2):
            re_v = prod[:RB, LN * half:LN * half + LN]
            im_v = prod[RB:, LN * half:LN * half + LN]
            if forward and mine:
                hats[layer, 0, half, t] = re_v
                hats[layer, 1, half, t] = im_v
            if not forward:
                re_v, im_v = re_v * cos_d + im_v * sin_d, im_v * cos_d - re_v * sin_d
            for ri, items in enumerate((re_v, im_v)):
                items = butterfly(items.reshape(16, 8, LN), range(4)).reshape(8, 2, 8, LN)
                for b6 in range(2):
                    tmp[64 * b6:64 * b6 + 64] = items[:, b6].reshape(64, LN)
                items = [tmp[pl.ds(m, 16, stride=8), :].reshape(2, 1, 8, LN) for m in range(8)]
                items = butterfly(jnp.concatenate(items, axis=1).reshape(16, 8, LN), range(3))
                work[ri, half, i] = items.reshape(RB, LN)

    def inner(layer, forward):
        slots = (0, 1, 0, 1, 2)

        def body(mine):
            def both(i, slot, after):
                prod = stage_mm(i, slot, layer, forward, mine)
                stage_in(i + 1, after, layer, forward, mine)
                stage_out(prod, i, layer, forward, mine)

            def trip(p, carry):
                i = start + 5 * p
                for n in range(5):
                    both(i + n, slots[n], slots[(n + 1) % 5])
                return carry
            start = first if mine else second
            lax.fori_loop(0, 3, trip, 0)

        first = 16 * pos_x
        second = 16 - first
        stage_in(first, 0, layer, forward, True)
        body(True)
        prod = stage_mm(first + 15, 0, layer, forward, True)
        stage_in(second, 0, layer, forward, False)
        stage_out(prod, first + 15, layer, forward, True)
        body(False)
        stage_out(stage_mm(second + 15, 0, layer, forward, False), second + 15, layer, forward, False)

    def last_rows(i):
        for ri in range(2):
            for half in range(2):
                ref = chunk_of(work, ri, half, i)
                radix32(ref, ref)

    def pieces(i, kg):
        return pl.ds(kg * KG, KG), pl.ds(pl.multiple_of(i * CH, CH), CH)

    def mix_pair(own_re, own_im, oth_re, oth_im, cos_b, sin_b):
        return (cos_b * own_re + sin_b * oth_re, cos_b * own_im + sin_b * oth_im,
                cos_b * oth_re - sin_b * own_re, cos_b * oth_im - sin_b * own_im)

    def first_rows(i, received):
        for ri in range(2):
            ref = chunk_of(work, ri, core, i)
            radix32(ref, ref)
            dst = chunk_of(work, ri, other, i)
            radix32(rchunk_of(ri, i) if received else dst, dst)

    def give_credit():
        pl.semaphore_signal(credit, inc=1, device_id=near_core, device_id_type=MESH)

    give_credit()

    def send_layer(layer, initial, sin_b, cos_b):
        layout = layer % 2
        angle = (0.5 / math.pi) * gamma_ref[pos_y, layer]

        def send_body(mine):
            def one(n, carry):
                i = (n + 8 * pos_x) % NCH
                if not initial:
                    last_rows(i)

                def point(kg, carry2):
                    ks, rows = pieces(i, kg)
                    here = pieces(n, kg)[1]
                    state = []
                    for half in range(2):
                        sin_p, cos_p = sincos(angle * cost_half(layout, half, ks, rows))
                        if initial:
                            real, imag = frame(lane_ones + core + half)
                            re_v = cos_p * real + sin_p * imag
                            im_v = cos_p * imag - sin_p * real
                        else:
                            re_v = work[0, half, ks, rows, :]
                            im_v = work[1, half, ks, rows, :]
                            re_v, im_v = re_v * cos_p + im_v * sin_p, im_v * cos_p - re_v * sin_p
                            waves[layer - 1, 0, half, ks, rows, :] = cos_p
                            waves[layer - 1, 1, half, ks, rows, :] = sin_p
                            if mine:
                                phis[layer - 1, 0, half, ks, here, :] = re_v
                                phis[layer - 1, 1, half, ks, here, :] = im_v
                        state += [re_v, im_v]
                    state = mix_pair(*state, cos_b, sin_b)
                    for half in range(2):
                        for ri in range(2):
                            work[ri, half, ks, rows, :] = state[2 * half + ri]
                    return carry2

                lax.fori_loop(0, NK // KG, point, 0)
                exchange(i).start()
                return carry
            return one

        lax.fori_loop(0, NCH // 2, send_body(True), 0)
        lax.fori_loop(NCH // 2, NCH, send_body(False), 0)

    def forward_layer(layer, carry):
        make_dtab(layer, 1.0)
        make_rot(layer, 1.0)
        sin_b, cos_b = half_angle(layer)
        pl.semaphore_wait(credit, 1)

        @pl.when(layer == 0)
        def _():
            send_layer(layer, True, sin_b, cos_b)

        @pl.when(layer > 0)
        def _():
            send_layer(layer, False, sin_b, cos_b)

        def take_body(n, carry2):
            i = (n + 8 * pos_x) % NCH
            exchange(i).wait()
            first_rows(i, True)
            return carry2

        lax.fori_loop(0, NCH, take_body, 0)
        give_credit()
        inner(layer, True)
        return carry

    lax.fori_loop(0, 3, forward_layer, 0)

    def turn_body(i, carry):
        total = jnp.zeros((CH, LN), F32)
        for half in range(2):
            for ri in range(2):
                ref = chunk_of(work, ri, half, i)
                values = butterfly(ref[...], range(5))
                lam = values * cost_half(1, half, slice(None), pl.ds(pl.multiple_of(i * CH, CH), CH))
                total = total + jnp.sum(values * lam, axis=0)
                ref[...] = butterfly(lam, range(5))
        acc[0] += 0.5 * total
        return carry

    lax.fori_loop(0, NCH, turn_body, 0)

    def backward_layer(back, carry0):
        layer = 2 - back
        layout = layer % 2
        make_dtab(layer, -1.0)
        make_rot(layer, -1.0)
        sin_b, cos_b = half_angle(layer)
        sin_b = sin_b * (2 * core - 1).astype(F32)
        angle = (0.5 / math.pi) * gamma_ref[pos_y, layer]
        inner(layer, False)
        pl.semaphore_wait(credit, 1)
        count = NCH // 2 + (NCH // 2) * ((layer + 1) // 2)

        def back_send(n, carry):
            i = (n + 8 * pos_x) % NCH
            last_rows(i)
            exchange(i).start()
            return carry

        lax.fori_loop(0, count, back_send, 0)

        def back_take(mine, final):
            def one(n, carry):
                i = (n + 8 * pos_x) % NCH
                exchange(i).wait()

                def point(kg, sums):
                    ks, rows = pieces(i, kg)
                    here = pieces(n, kg)[1]
                    beta_sum, gamma_sum = sums
                    own_re = work[0, core, ks, rows, :]
                    own_im = work[1, core, ks, rows, :]
                    oth_re = recv[0, ks, rows, :]
                    oth_im = recv[1, ks, rows, :]
                    lam = mix_pair(own_re, own_im, oth_re, oth_im, cos_b, sin_b)
                    lams = (lam[:2], lam[2:])
                    if mine:
                        phi = []
                        costs = []
                        for side in (core, other):
                            cost_v = cost_half(layout, side, ks, rows)
                            costs.append(cost_v)
                            if final:
                                sin_p, cos_p = sincos(angle * cost_v)
                                real, imag = frame(lane_ones + core + side)
                                phi.append((cos_p * real + sin_p * imag, cos_p * imag - sin_p * real))
                            else:
                                phi.append((phis[layer - 1, 0, side, ks, here, :], phis[layer - 1, 1, side, ks, here, :]))
                        for side in range(2):
                            lam_re, lam_im = lams[side]
                            gamma_sum = gamma_sum + jnp.sum(costs[side] * (lam_re * phi[side][1] - lam_im * phi[side][0]), axis=0)
                            cross = jnp.sum(lam_re * phi[1 - side][0] + lam_im * phi[1 - side][1], axis=0)
                            beta_sum = beta_sum + cross if side == 0 else beta_sum - cross
                    if not final:
                        for side, where in enumerate((core, other)):
                            lam_re, lam_im = lams[side]
                            cos_p = waves[layer - 1, 0, where, ks, rows, :]
                            sin_p = waves[layer - 1, 1, where, ks, rows, :]
                            work[0, where, ks, rows, :] = lam_re * cos_p - lam_im * sin_p
                            work[1, where, ks, rows, :] = lam_im * cos_p + lam_re * sin_p
                    return beta_sum, gamma_sum

                zero = jnp.zeros((CH, LN), F32)
                beta_sum, gamma_sum = lax.fori_loop(0, NK // KG, point, (zero, zero))
                if mine:
                    acc[1 + layer] += beta_sum * (1 - 2 * core).astype(F32)
                    acc[4 + layer] += 2.0 * gamma_sum
                if not final:
                    first_rows(i, False)
                return carry
            return one

        @pl.when(layer > 0)
        def _():
            lax.fori_loop(0, NCH // 2, back_take(True, False), 0)
            lax.fori_loop(NCH // 2, NCH, back_take(False, False), 0)

        @pl.when(layer == 0)
        def _():
            lax.fori_loop(0, NCH // 2, back_take(True, True), 0)

        give_credit()
        return carry0

    lax.fori_loop(0, 3, backward_layer, 0)
    pl.semaphore_wait(credit, 1)

    order = (0, 4, 5, 6, 1, 2, 3)
    rows = [jnp.sum(acc[q], axis=0, keepdims=True) for q in order]
    part[...] = jnp.concatenate(rows + [jnp.zeros((1, LN), F32)], axis=0)
    peers[pos_y, pos_b] = part[...]
    fins = [push(part, peers.at[pos_y, pos_b], fin_s.at[n], fin_r.at[n], dev) for n, dev in enumerate(others)]
    for copy in fins:
        copy.start()
    for copy in fins:
        copy.wait()
    for n in range(2):
        total = peers[n, 0] + peers[n, 1] + peers[n, 2] + peers[n, 3]
        for q in range(7):
            value = jnp.sum(total[q:q + 1])
            if q == 0:
                energy_ref[n] = value
            else:
                grad_ref[n, q - 1] = value


def solution(mesh):
    def device_fn(cost, gamma, beta):
        vmem = pl.BlockSpec(memory_space=pltpu.VMEM)
        smem = pl.BlockSpec(memory_space=pltpu.SMEM)
        dma = pltpu.SemaphoreType.DMA
        return pl.pallas_call(
            kernel,
            out_shape=(jax.ShapeDtypeStruct((2,), F32), jax.ShapeDtypeStruct((2, 6), F32)),
            in_specs=[vmem, smem, smem],
            out_specs=(smem, smem),
            scratch_shapes=[
                pltpu.VMEM((2, 2, NK, RB, LN), F32),
                pltpu.VMEM((2, 2, NK, RB, LN), F32),
                pltpu.VMEM((2, NK, RB, LN), F32),
                pltpu.VMEM((3, 2, 2, NK // 2, RB, LN), F32),
                pltpu.VMEM((2, 2, 2, NK, RB // 2, LN), F32),
                pltpu.VMEM((2, 2, 2, NK, RB, LN), F32),
                pltpu.VMEM((768, 256), BF16),
                pltpu.VMEM((256, 256), BF16),
                pltpu.VMEM((RB, LN), F32),
                pltpu.VMEM((3, 256, 768), BF16),
                pltpu.VMEM((2, 10, 8, LN), F32),
                pltpu.VMEM((8, LN), F32),
                pltpu.VMEM((8, 8, LN), F32),
                pltpu.VMEM((8, LN), F32),
                pltpu.VMEM((2, 4, 8, LN), F32),
                dma((2, 4)), dma((2, 4)), dma((4,)), dma((4,)), dma((4, 4)), dma((4, 4)),
                dma((NCH,)), dma((NCH,)), dma((7,)), dma((7,)),
                pltpu.SemaphoreType.REGULAR,
            ],
            compiler_params=pltpu.CompilerParams(collective_id=0, has_side_effects=True, vmem_limit_bytes=67043328),
        )(cost.reshape(16, RB, LN), gamma, beta)

    cost_spec = P(('inst', 'qy', 'qx'))
    angle_spec = P('inst', None)
    return jax.shard_map(device_fn, mesh=mesh, in_specs=(cost_spec, angle_spec, angle_spec), out_specs=(P('inst'), angle_spec), check_vma=False)
```

```python
import functools
import math
import jax
import jax.numpy as jnp
from jax import lax
from jax.experimental import pallas as pl
from jax.experimental.pallas import tpu as pltpu
from jax.sharding import PartitionSpec as P

F32 = jnp.float32
BF16 = jnp.bfloat16
NK = 32
RB = 128
LN = 128
CH = 8
NCH = RB // CH
GC = 4
KG = 4
MESH = pl.DeviceIdType.MESH
QUBITS = 21
ROWQ = 12


def popcount(value, bits):
    total = value % 2
    for bit in range(1, bits):
        total = total + (value // 2 ** bit) % 2
    return total


def sincos(turns):
    frac = turns - jnp.round(turns)
    sq = frac * frac
    sin_h = 1.098257528e-01
    sin_h = sin_h * sq - 8.461123459e-01
    sin_h = sin_h * sq + 3.606354339e+00
    sin_h = sin_h * sq - 7.308245693e+00
    sin_h = sin_h * sq + 4.442882919e+00
    sin_h = sin_h * frac
    cos_h = -3.450177884e-02
    cos_h = cos_h * sq + 3.322516636e-01
    cos_h = cos_h * sq - 1.888274957e+00
    cos_h = cos_h * sq + 5.739881543e+00
    cos_h = cos_h * sq - 6.978864110e+00
    cos_h = cos_h * sq + 1.414213562e+00
    return sin_h * cos_h, 1.0 - sin_h * sin_h


def butterfly(items, bits):
    shape = items.shape
    for bit in bits:
        step = 1 << bit
        pairs = items.reshape((shape[0] // (2 * step), 2, step) + shape[1:])
        first = pairs[:, 0]
        second = pairs[:, 1]
        items = jnp.stack([first + second, first - second], axis=1).reshape(shape)
    return items


def split(values):
    high = values.astype(BF16)
    rest = values - high.astype(F32)
    mid = rest.astype(BF16)
    return high, mid, (rest - mid.astype(F32)).astype(BF16)


def kernel(cost_ref, gamma_ref, beta_ref, energy_ref, grad_ref, cost_all, work, recv, hats, phis, waves, rot, flip, tmp, lhs, dtab, wtab, acc, part, peers,
           own_s, own_r, rel_s, rel_r, core_s, core_r, ex_s, ex_r, fin_s, fin_r, credit):
    pos_y = lax.axis_index('qy')
    pos_b = lax.axis_index('qx')
    pos_x = pos_b // 2
    core = pos_b % 2
    other = 1 - core
    near_core = {'qy': pos_y, 'qx': pos_x * 2 + other}
    near_x = {'qy': pos_y, 'qx': (1 - pos_x) * 2 + core}
    near_y = {'qy': 1 - pos_y, 'qx': pos_b}
    others = []
    for d in range(1, 8):
        to_y = 1 - pos_y if d & 4 else pos_y
        to_x = 1 - pos_x if d & 2 else pos_x
        to_core = other if d & 1 else core
        others.append({'qy': to_y, 'qx': to_x * 2 + to_core})

    barrier = pltpu.get_barrier_semaphore()
    for dev in others:
        pl.semaphore_signal(barrier, inc=1, device_id=dev, device_id_type=MESH)
    pl.semaphore_wait(barrier, 7)

    def slot(block_y, block_x, block_core, chunk):
        return cost_all.at[block_y, block_x, pl.ds(block_core * 16 + chunk * GC, GC)]

    def push(src, dst, send, rcv, dev):
        return pltpu.make_async_remote_copy(src_ref=src, dst_ref=dst, send_sem=send, recv_sem=rcv, device_id=dev, device_id_type=MESH)

    sends = []

    def go(copy):
        copy.start()
        sends.append(copy)

    for q in range(4):
        src = cost_ref.at[pl.ds(q * GC, GC)]
        dst = slot(pos_y, pos_x, core, q)
        go(push(src, dst, own_s.at[0, q], own_r.at[0, q], near_x))
        go(push(src, dst, own_s.at[1, q], own_r.at[1, q], near_y))
        go(push(src, dst, core_s.at[0, q], core_r.at[0, q], near_core))

    cost_all[pos_y, pos_x, pl.ds(core * 16, 16)] = cost_ref[...]

    row_i = lax.broadcasted_iota(jnp.int32, (256, 256), 0)
    col_i = lax.broadcasted_iota(jnp.int32, (256, 256), 1)
    differ = row_i ^ col_i
    single = (differ != 0) & ((differ & (differ - 1)) == 0)
    flip_v = jnp.where(single, jnp.where(row_i > col_i, 1.0, -1.0), 0.0).astype(BF16)
    flip[...] = flip_v
    lane_i = lax.broadcasted_iota(jnp.int32, (8, LN), 1)
    sub_i = lax.broadcasted_iota(jnp.int32, (8, LN), 0)
    wtab[...] = (ROWQ - 2 * popcount(sub_i, 3)).astype(F32)
    lane_ones = popcount(lane_i, 7)
    acc[...] = jnp.zeros_like(acc)

    for q in range(4):
        block = slot(pos_y, 1 - pos_x, core, q)
        push(block, block, own_s.at[0, q], own_r.at[0, q], near_x).wait_recv()
        go(push(block, block, core_s.at[1, q], core_r.at[1, q], near_core))
        if q < 2:
            go(push(block, block, rel_s.at[q], rel_r.at[q], near_y))
        block = slot(1 - pos_y, pos_x, core, q)
        push(block, block, own_s.at[1, q], own_r.at[1, q], near_y).wait_recv()
        go(push(block, block, core_s.at[2, q], core_r.at[2, q], near_core))
        if q >= 2:
            go(push(block, block, rel_s.at[q], rel_r.at[q], near_x))
    for q in (0, 2, 1, 3):
        block = slot(1 - pos_y, 1 - pos_x, core, q)
        push(block, block, rel_s.at[q], rel_r.at[q], near_x).wait_recv()
        go(push(block, block, core_s.at[3, q], core_r.at[3, q], near_core))
    for q in range(4):
        for kind, (by, bx) in enumerate(((pos_y, pos_x), (pos_y, 1 - pos_x), (1 - pos_y, pos_x), (1 - pos_y, 1 - pos_x))):
            block = slot(by, bx, other, q)
            push(block, block, core_s.at[kind, q], core_r.at[kind, q], near_core).wait_recv()
    for copy in sends:
        copy.wait_send()

    def make_dtab(layer, sign):
        half = (0.25 / math.pi) * beta_ref[pos_y, layer]
        for pop in range(10):
            sin_v, cos_v = sincos(half * (wtab[...] - 2.0 * pop))
            dtab[0, pop] = cos_v * 2.0 ** -ROWQ
            dtab[1, pop] = sin_v * (sign * 2.0 ** -ROWQ)

    def half_angle(layer):
        return sincos(jnp.full((1, CH, LN), (0.25 / math.pi) * beta_ref[pos_y, layer], F32))

    def make_rot(layer, sign):
        sin_b, cos_b = sincos(jnp.full((8, 256), (0.25 / math.pi) * beta_ref[pos_y, layer], F32))
        sin_b = sin_b * sign
        cols = lax.broadcasted_iota(jnp.int32, (8, 256), 1)

        def body(n, carry):
            tiles = []
            for sub in range(2):
                lines = lax.broadcasted_iota(jnp.int32, (8, 256), 0) + n * 16 + sub * 8
                delta = lines ^ cols
                total = None
                for bit in range(8):
                    factor = jnp.where((delta >> bit) & 1 == 0, cos_b, jnp.where((lines >> bit) & 1 == 1, sin_b, -sin_b))
                    total = factor if total is None else total * factor
                tiles.append(total)
            high, mid, low = split(jnp.concatenate(tiles, axis=0))
            for m, piece in enumerate((high, mid, low)):
                rot[pl.ds(pl.multiple_of(m * 256 + n * 16, 16), 16), :] = piece
            return carry

        lax.fori_loop(0, 16, body, 0)

    def frame(ones):
        turn = ones % 4
        real = jnp.where(turn == 0, 1.0, jnp.where(turn == 2, -1.0, 0.0))
        imag = jnp.where(turn == 1, -1.0, jnp.where(turn == 3, 1.0, 0.0))
        scale = 2.0 ** (-0.5 * QUBITS)
        return real[None] * scale, imag[None] * scale

    def cost_half(layout, half, ks, rows):
        return cost_all[(1 - layout) * core + layout * half, (1 - layout) * half + layout * core, ks, rows, :]

    def radix32(src, dst):
        dst[...] = butterfly(src[...], range(5))

    def chunk_of(ref, ri, half, i):
        return ref.at[ri, half, :, pl.ds(pl.multiple_of(i * CH, CH), CH), :]

    def rchunk_of(ri, i):
        return recv.at[ri, :, pl.ds(pl.multiple_of(i * CH, CH), CH), :]

    def exchange(i):
        rows = pl.ds(pl.multiple_of(i * CH, CH), CH)
        return push(work.at[:, other, :, rows, :], recv.at[:, :, rows, :], ex_s.at[i], ex_r.at[i], near_core)

    def row_wave(i):
        pop_i = popcount(jnp.asarray(i, jnp.int32), 5)
        pops = [bin(m).count('1') for m in range(16)]
        return [jnp.concatenate([dtab[n, pop_i + pop] for pop in pops], axis=0) for n in range(2)]

    def stage_in(i, slot, layer, forward, mine):
        t = i - 16 * pos_x
        if forward:
            cos_d, sin_d = row_wave(i)
        for half in range(2):
            pair = []
            for ri in range(2):
                items = butterfly(work[ri, half, i].reshape(16, 8, LN), range(3))
                tmp[...] = items.reshape(RB, LN)
                items = [tmp[pl.ds(m, 16, stride=8), :].reshape(1, 2, 8, LN) for m in range(8)]
                pair.append(butterfly(jnp.concatenate(items, axis=0).reshape(16, 8, LN), range(4)).reshape(RB, LN))
            re_v, im_v = pair
            if forward:
                pair = [re_v * cos_d + im_v * sin_d, im_v * cos_d - re_v * sin_d]
            elif mine:
                prod = re_v * hats[layer, 1, half, t] - im_v * hats[layer, 0, half, t]
                sums = [None] * 5
                for m in range(16):
                    pop = bin(m).count('1')
                    piece = prod[8 * m:8 * m + 8]
                    sums[pop] = piece if sums[pop] is None else sums[pop] + piece
                flat = sums[0] + sums[1] + sums[2] + sums[3] + sums[4]
                tilt = sums[1] + 2.0 * sums[2] + 3.0 * sums[3] + 4.0 * sums[4]
                pop_i = popcount(jnp.asarray(i, jnp.int32), 5)
                acc[1 + layer] += (wtab[...] - 2.0 * jnp.asarray(pop_i, F32)) * flat - 2.0 * tilt
            for ri in range(2):
                for n, piece in enumerate(split(pair[ri])):
                    lhs[slot, pl.ds(RB * ri, RB), pl.ds(2 * LN * n + LN * half, LN)] = piece

    def stage_mm(i, slot, layer, forward, mine):
        t = i - 16 * pos_x
        high = lhs[slot, :, 0:256]
        mid = lhs[slot, :, 256:512]
        low = lhs[slot, :, 512:768]
        table = jnp.concatenate([rot[...], rot[0:512], rot[0:256]], axis=0)
        parts = jnp.concatenate([high, high, high, mid, mid, low], axis=1)
        prods = []
        for ri in range(2):
            prods.append(jnp.dot(parts[RB * ri:RB * ri + RB], table, preferred_element_type=F32))
        prod = jnp.concatenate(prods, axis=0)
        if not forward and mine:
            turned = jnp.dot(jnp.concatenate([high, mid, low], axis=1), jnp.concatenate([flip[...]] * 3, axis=0), preferred_element_type=F32)
            total = None
            for half in range(2):
                for ri in range(2):
                    piece = turned[RB * ri:RB * ri + RB, LN * half:LN * half + LN] * hats[layer, ri, half, t]
                    piece = jnp.sum(piece.reshape(16, 8, LN), axis=0)
                    total = piece if total is None else total + piece
            acc[1 + layer] -= total
        return prod

    def stage_out(prod, i, layer, forward, mine):
        t = i - 16 * pos_x
        if not forward:
            cos_d, sin_d = row_wave(i)
        for half in range(2):
            re_v = prod[:RB, LN * half:LN * half + LN]
            im_v = prod[RB:, LN * half:LN * half + LN]
            if forward and mine:
                hats[layer, 0, half, t] = re_v
                hats[layer, 1, half, t] = im_v
            if not forward:
                re_v, im_v = re_v * cos_d + im_v * sin_d, im_v * cos_d - re_v * sin_d
            for ri, items in enumerate((re_v, im_v)):
                items = butterfly(items.reshape(16, 8, LN), range(4)).reshape(8, 2, 8, LN)
                for b6 in range(2):
                    tmp[64 * b6:64 * b6 + 64] = items[:, b6].reshape(64, LN)
                items = [tmp[pl.ds(m, 16, stride=8), :].reshape(2, 1, 8, LN) for m in range(8)]
                items = butterfly(jnp.concatenate(items, axis=1).reshape(16, 8, LN), range(3))
                work[ri, half, i] = items.reshape(RB, LN)

    def inner(layer, forward):
        slots = (0, 1, 0, 1, 2)

        def body(mine):
            def both(i, slot, after):
                prod = stage_mm(i, slot, layer, forward, mine)
                stage_in(i + 1, after, layer, forward, mine)
                stage_out(prod, i, layer, forward, mine)

            def trip(p, carry):
                i = start + 5 * p
                for n in range(5):
                    both(i + n, slots[n], slots[(n + 1) % 5])
                return carry
            start = first if mine else second
            lax.fori_loop(0, 3, trip, 0)

        first = 16 * pos_x
        second = 16 - first
        stage_in(first, 0, layer, forward, True)
        body(True)
        prod = stage_mm(first + 15, 0, layer, forward, True)
        stage_in(second, 0, layer, forward, False)
        stage_out(prod, first + 15, layer, forward, True)
        body(False)
        stage_out(stage_mm(second + 15, 0, layer, forward, False), second + 15, layer, forward, False)

    def last_rows(i):
        for ri in range(2):
            for half in range(2):
                ref = chunk_of(work, ri, half, i)
                radix32(ref, ref)

    def pieces(i, kg):
        return pl.ds(kg * KG, KG), pl.ds(pl.multiple_of(i * CH, CH), CH)

    def mix_pair(own_re, own_im, oth_re, oth_im, cos_b, sin_b):
        return (cos_b * own_re + sin_b * oth_re, cos_b * own_im + sin_b * oth_im,
                cos_b * oth_re - sin_b * own_re, cos_b * oth_im - sin_b * own_im)

    def first_rows(i, received):
        for ri in range(2):
            ref = chunk_of(work, ri, core, i)
            radix32(ref, ref)
            dst = chunk_of(work, ri, other, i)
            radix32(rchunk_of(ri, i) if received else dst, dst)

    def give_credit():
        pl.semaphore_signal(credit, inc=1, device_id=near_core, device_id_type=MESH)

    give_credit()

    def send_layer(layer, initial, sin_b, cos_b):
        layout = layer % 2
        angle = (0.5 / math.pi) * gamma_ref[pos_y, layer]

        def send_body(mine):
            def one(n, carry):
                i = (n + 8 * pos_x) % NCH
                if not initial:
                    last_rows(i)

                def point(kg, carry2):
                    ks, rows = pieces(i, kg)
                    here = pieces(n, kg)[1]
                    state = []
                    for half in range(2):
                        sin_p, cos_p = sincos(angle * cost_half(layout, half, ks, rows))
                        if initial:
                            real, imag = frame(lane_ones + core + half)
                            re_v = cos_p * real + sin_p * imag
                            im_v = cos_p * imag - sin_p * real
                        else:
                            re_v = work[0, half, ks, rows, :]
                            im_v = work[1, half, ks, rows, :]
                            re_v, im_v = re_v * cos_p + im_v * sin_p, im_v * cos_p - re_v * sin_p
                            waves[layer - 1, 0, half, ks, rows, :] = cos_p
                            waves[layer - 1, 1, half, ks, rows, :] = sin_p
                            if mine:
                                phis[layer - 1, 0, half, ks, here, :] = re_v
                                phis[layer - 1, 1, half, ks, here, :] = im_v
                        state += [re_v, im_v]
                    state = mix_pair(*state, cos_b, sin_b)
                    for half in range(2):
                        for ri in range(2):
                            work[ri, half, ks, rows, :] = state[2 * half + ri]
                    return carry2

                lax.fori_loop(0, NK // KG, point, 0)
                exchange(i).start()
                return carry
            return one

        lax.fori_loop(0, NCH // 2, send_body(True), 0)
        lax.fori_loop(NCH // 2, NCH, send_body(False), 0)

    def forward_layer(layer, carry):
        make_dtab(layer, 1.0)
        make_rot(layer, 1.0)
        sin_b, cos_b = half_angle(layer)
        pl.semaphore_wait(credit, 1)

        @pl.when(layer == 0)
        def _():
            send_layer(layer, True, sin_b, cos_b)

        @pl.when(layer > 0)
        def _():
            send_layer(layer, False, sin_b, cos_b)

        def take_body(n, carry2):
            i = (n + 8 * pos_x) % NCH
            exchange(i).wait()
            first_rows(i, True)
            return carry2

        lax.fori_loop(0, NCH, take_body, 0)
        give_credit()
        inner(layer, True)
        return carry

    lax.fori_loop(0, 3, forward_layer, 0)

    def turn_body(i, carry):
        total = jnp.zeros((CH, LN), F32)
        for half in range(2):
            for ri in range(2):
                ref = chunk_of(work, ri, half, i)
                values = butterfly(ref[...], range(5))
                lam = values * cost_half(1, half, slice(None), pl.ds(pl.multiple_of(i * CH, CH), CH))
                total = total + jnp.sum(values * lam, axis=0)
                ref[...] = butterfly(lam, range(5))
        acc[0] += 0.5 * total
        return carry

    lax.fori_loop(0, NCH, turn_body, 0)

    def backward_layer(back, carry0):
        layer = 2 - back
        layout = layer % 2
        make_dtab(layer, -1.0)
        make_rot(layer, -1.0)
        sin_b, cos_b = half_angle(layer)
        sin_b = sin_b * (2 * core - 1).astype(F32)
        angle = (0.5 / math.pi) * gamma_ref[pos_y, layer]
        inner(layer, False)
        pl.semaphore_wait(credit, 1)
        count = NCH // 2 + (NCH // 2) * ((layer + 1) // 2)

        def back_send(n, carry):
            i = (n + 8 * pos_x) % NCH
            last_rows(i)
            exchange(i).start()
            return carry

        lax.fori_loop(0, count, back_send, 0)

        def back_take(mine, final):
            def one(n, carry):
                i = (n + 8 * pos_x) % NCH
                exchange(i).wait()

                def point(kg, sums):
                    ks, rows = pieces(i, kg)
                    here = pieces(n, kg)[1]
                    beta_sum, gamma_sum = sums
                    own_re = work[0, core, ks, rows, :]
                    own_im = work[1, core, ks, rows, :]
                    oth_re = recv[0, ks, rows, :]
                    oth_im = recv[1, ks, rows, :]
                    lam = mix_pair(own_re, own_im, oth_re, oth_im, cos_b, sin_b)
                    lams = (lam[:2], lam[2:])
                    if mine:
                        phi = []
                        costs = []
                        for side in (core, other):
                            cost_v = cost_half(layout, side, ks, rows)
                            costs.append(cost_v)
                            if final:
                                sin_p, cos_p = sincos(angle * cost_v)
                                real, imag = frame(lane_ones + core + side)
                                phi.append((cos_p * real + sin_p * imag, cos_p * imag - sin_p * real))
                            else:
                                phi.append((phis[layer - 1, 0, side, ks, here, :], phis[layer - 1, 1, side, ks, here, :]))
                        for side in range(2):
                            lam_re, lam_im = lams[side]
                            gamma_sum = gamma_sum + jnp.sum(costs[side] * (lam_re * phi[side][1] - lam_im * phi[side][0]), axis=0)
                            cross = jnp.sum(lam_re * phi[1 - side][0] + lam_im * phi[1 - side][1], axis=0)
                            beta_sum = beta_sum + cross if side == 0 else beta_sum - cross
                    if not final:
                        for side, where in enumerate((core, other)):
                            lam_re, lam_im = lams[side]
                            cos_p = waves[layer - 1, 0, where, ks, rows, :]
                            sin_p = waves[layer - 1, 1, where, ks, rows, :]
                            work[0, where, ks, rows, :] = lam_re * cos_p - lam_im * sin_p
                            work[1, where, ks, rows, :] = lam_im * cos_p + lam_re * sin_p
                    return beta_sum, gamma_sum

                zero = jnp.zeros((CH, LN), F32)
                beta_sum, gamma_sum = lax.fori_loop(0, NK // KG, point, (zero, zero))
                if mine:
                    acc[1 + layer] += beta_sum * (1 - 2 * core).astype(F32)
                    acc[4 + layer] += 2.0 * gamma_sum
                if not final:
                    first_rows(i, False)
                return carry
            return one

        @pl.when(layer > 0)
        def _():
            lax.fori_loop(0, NCH // 2, back_take(True, False), 0)
            lax.fori_loop(NCH // 2, NCH, back_take(False, False), 0)

        @pl.when(layer == 0)
        def _():
            lax.fori_loop(0, NCH // 2, back_take(True, True), 0)

        give_credit()
        return carry0

    lax.fori_loop(0, 3, backward_layer, 0)
    pl.semaphore_wait(credit, 1)

    order = (0, 4, 5, 6, 1, 2, 3)
    rows = [jnp.sum(acc[q], axis=0, keepdims=True) for q in order]
    part[...] = jnp.concatenate(rows + [jnp.zeros((1, LN), F32)], axis=0)
    peers[pos_y, pos_b] = part[...]
    fins = [push(part, peers.at[pos_y, pos_b], fin_s.at[n], fin_r.at[n], dev) for n, dev in enumerate(others)]
    for copy in fins:
        copy.start()
    for copy in fins:
        copy.wait()
    for n in range(2):
        total = peers[n, 0] + peers[n, 1] + peers[n, 2] + peers[n, 3]
        for q in range(7):
            value = jnp.sum(total[q:q + 1])
            if q == 0:
                energy_ref[n] = value
            else:
                grad_ref[n, q - 1] = value


def solution(mesh):
    def device_fn(cost, gamma, beta):
        vmem = pl.BlockSpec(memory_space=pltpu.VMEM)
        smem = pl.BlockSpec(memory_space=pltpu.SMEM)
        dma = pltpu.SemaphoreType.DMA
        return pl.pallas_call(
            kernel,
            out_shape=(jax.ShapeDtypeStruct((2,), F32), jax.ShapeDtypeStruct((2, 6), F32)),
            in_specs=[vmem, smem, smem],
            out_specs=(smem, smem),
            scratch_shapes=[
                pltpu.VMEM((2, 2, NK, RB, LN), F32),
                pltpu.VMEM((2, 2, NK, RB, LN), F32),
                pltpu.VMEM((2, NK, RB, LN), F32),
                pltpu.VMEM((3, 2, 2, NK // 2, RB, LN), F32),
                pltpu.VMEM((2, 2, 2, NK, RB // 2, LN), F32),
                pltpu.VMEM((2, 2, 2, NK, RB, LN), F32),
                pltpu.VMEM((768, 256), BF16),
                pltpu.VMEM((256, 256), BF16),
                pltpu.VMEM((RB, LN), F32),
                pltpu.VMEM((3, 256, 768), BF16),
                pltpu.VMEM((2, 10, 8, LN), F32),
                pltpu.VMEM((8, LN), F32),
                pltpu.VMEM((8, 8, LN), F32),
                pltpu.VMEM((8, LN), F32),
                pltpu.VMEM((2, 4, 8, LN), F32),
                dma((2, 4)), dma((2, 4)), dma((4,)), dma((4,)), dma((4, 4)), dma((4, 4)),
                dma((NCH,)), dma((NCH,)), dma((7,)), dma((7,)),
                pltpu.SemaphoreType.REGULAR,
            ],
            compiler_params=pltpu.CompilerParams(collective_id=0, has_side_effects=True, vmem_limit_bytes=67043328),
        )(cost.reshape(16, RB, LN), gamma, beta)

    cost_spec = P(('inst', 'qy', 'qx'))
    angle_spec = P('inst', None)
    return jax.shard_map(device_fn, mesh=mesh, in_specs=(cost_spec, angle_spec, angle_spec), out_specs=(P('inst'), angle_spec), check_vma=False)
```
